1024 devices in a mesh: dom: 64 (over y, z_lo, core), band: 16 (over x, z_hi).
Axes of the slice: x: 4, y: 4, z: 32 (z_hi: 4, z_lo: 8; z = z_hi * 8 + z_lo), core: 2. Of those that a mesh axis runs over, the one named last changes fastest.
Arguments:
- wavefunctions: bfloat16 [32768, 2048], P('dom', 'band'), may hold values from -6 to 6
- cell_ham: bfloat16 [128, 512, 512], P('dom'), may hold values from -0.25 to 0.25
- connectivity: int32 [128, 512], P('dom'), may hold values from 0 to 767, as said below
- inv_mass: float32 [32768], P('dom'), may hold values from 0.5 to 2
- cell_count: int32 [64], P('dom'), may hold values from 1 to 2, as said below
Outputs:
- filtered: bfloat16 [32768, 2048], P('dom', 'band')
- margin: float32 [2048, 2048], P('band', 'dom')
The draws below stay inside these ranges and needn't reach their ends.
Inputs may be any that keep to these rules, and one draw needn't show every extreme that they name: `connectivity`: row c of domain d lists 512 indices into that domain's nodes extended by 128 nodes on each side; every extended index appears in some row of its domain. `cell_count`: some domain has all 2 cells live in every draw.
All inputs are finite; a program needn't handle non-finite values.
Results may differ from the reference program's by a relative error of at most 0.0052.
Values may be sent and summed in bfloat16 or wider, within the bound.
A program may use at most 32 MiB of HBM per device.

```python
import math
import jax
import jax.numpy as jnp
from jax import lax

NPC = 512
CELLS_DEV = 2
DEGREE = 4
NODES_DEV = 512
GHOST = 128
NODES = 32768
CELLS = 128
NBANDS = 2048
N_DOM = 64


def draw_connectivity(key, part):
    domains = CELLS // CELLS_DEV
    extended = NODES_DEV + 2 * GHOST
    slots = CELLS_DEV * NPC

    def single(subkey):
        first, second, third = jax.random.split(subkey, 3)
        base = jax.random.permutation(first, extended)
        extra = jax.random.randint(second, (slots - extended,), 0, extended)
        joined = jnp.concatenate([base, extra])
        joined = jax.random.permutation(third, joined)
        return joined.reshape(CELLS_DEV, NPC)
    keys = jax.random.split(jax.random.fold_in(key, 11), domains)
    return jax.vmap(single)(keys).reshape(CELLS, NPC).astype(jnp.int32)


def draw_cell_count(key, part):
    domains = NODES // NODES_DEV
    first, second = jax.random.split(jax.random.fold_in(key, 23))
    lowest = max(1, CELLS_DEV // 2)
    counts = jax.random.randint(first, (domains,), lowest, CELLS_DEV + 1)
    chosen = jax.random.randint(second, (), 0, domains)
    counts = jnp.where(jnp.arange(domains) == chosen, CELLS_DEV, counts)
    return counts.astype(jnp.int32)


def levels(rng, shape, cuts, low, largest):
    def one(position, shards_of):
        steps = jax.random.uniform(jax.random.fold_in(jax.random.fold_in(rng, 6), position), (shards_of,), jnp.float32, low / len(cuts), largest / len(cuts))
        return jnp.repeat(jnp.exp(steps), shape[position] // shards_of).reshape((-1,) + (1,) * (len(shape) - position - 1))

    factor_of = one(*cuts[0])
    for cut in cuts[1:]:
        factor_of = factor_of * one(*cut)
    return factor_of


def normal_values(key, dims, scale, limit, cuts=(), held_as=jnp.bfloat16):
    factor_of = levels(key, dims, cuts, -0.22, 0.18) if cuts else 1.0
    values = jax.random.normal(key, dims, jnp.float32) * scale * factor_of
    return jnp.minimum(jnp.maximum(values, -limit), limit).astype(held_as)


def setup_inputs(seed: int = 0) -> dict:
    seeds = jax.random.split(jax.random.key(seed), 6)
    return {
        "wavefunctions": normal_values(seeds[0], (NODES, NBANDS), 1.0, 6.0, ((0, 64), (1, 16))),
        "cell_ham": normal_values(seeds[1], (CELLS, NPC, NPC), NPC ** -0.5, 0.25, ((0, 64),)),
        "connectivity": draw_connectivity(jax.random.fold_in(seeds[5], 71), 0),
        "inv_mass": jnp.clip(jnp.exp(math.log(2.0) - 1.3862944 * jax.random.uniform(seeds[3], (NODES,), jnp.float32) ** levels(seeds[3], (NODES,), ((0, 64),), -0.2, 0.2)), 0.5, 2.0),
        "cell_count": draw_cell_count(jax.random.fold_in(seeds[5], 71), 0),
    }


filter_center = 0.5
filter_halfwidth = 3.0

def apply_operator(current, cell_ham, connectivity, inv_mass, cell_count):
    values = current.astype(jnp.bfloat16)

    def per_domain(total, domain):
        hams = lax.dynamic_slice_in_dim(cell_ham, domain * CELLS_DEV, CELLS_DEV, 0)
        conn = lax.dynamic_slice_in_dim(connectivity, domain * CELLS_DEV, CELLS_DEV, 0)
        glob = jnp.mod(domain * NODES_DEV + conn - GHOST, NODES).astype(jnp.int32)
        taken = values[glob]
        prod = jnp.einsum('cij,cjb->cib', hams.astype(jnp.float32), taken.astype(jnp.float32))
        live = (jnp.arange(CELLS_DEV, dtype=jnp.int32) < cell_count[domain]).astype(jnp.float32)
        prod = prod * live[:, None, None]
        total = total.at[glob.reshape(-1)].add(prod.reshape(-1, prod.shape[-1]))
        return (total, None)
    start = jnp.zeros(current.shape, jnp.float32)
    total, unused = lax.scan(per_domain, start, jnp.arange(N_DOM, dtype=jnp.int32))
    return inv_mass[:, None] * total

def reference(wavefunctions, cell_ham, connectivity, inv_mass, cell_count):

    def operate(field):
        return apply_operator(field, cell_ham, connectivity, inv_mass, cell_count)
    previous = wavefunctions.astype(jnp.float32)
    current = (operate(previous) - filter_center * previous) / filter_halfwidth
    for step in range(DEGREE - 1):
        following = 2.0 * (operate(current) - filter_center * current) / filter_halfwidth - previous
        previous = current
        current = following
    filtered = current.astype(jnp.bfloat16)
    gram = jnp.dot(filtered.T, filtered, preferred_element_type=jnp.float32)
    margin = gram * (1.0 / jnp.sqrt(jnp.float32(NODES)))
    return (filtered, margin)
```

```python
import functools

import jax
import jax.numpy as jnp
from jax import lax
from jax.experimental import pallas as pl
from jax.experimental.pallas import tpu as pltpu
from jax.sharding import PartitionSpec as P

DEGREE = 4
CENTER = 0.5
HALFWIDTH = 3.0
NX, NY, NH, NZ = 4, 4, 4, 8
MESH = pl.DeviceIdType.MESH


def tile_of(size, most):
    return most if size % most == 0 else size


def kernel(
    shape, w_ref, h_ref, conn_ref, im_ref, cnt_ref, filt_ref, marg_ref,
    st, thi, tlo, ahi, alo, mext, imx, vext, ys, us_f, us, ur, rb, lb, pacc,
    es, er, zs, zr,
    s_w, r_w, s_im, r_im, s_u, r_u, s_r, r_r, s_l, r_l, s_e, r_e, s_z, r_z,
):
    nx, ny, nh, nz = shape
    own, width = w_ref.shape
    cells, npc, _ = h_ref.shape
    ghost = own // 4
    ext = own + 2 * ghost
    block = 2 * ghost
    hh = nh // 2
    out_rows = width // 4
    domains = ny * nz * 2

    d = lax.axis_index("dom")
    b = lax.axis_index("band")
    c = lax.rem(d, 2)
    zl = lax.rem(lax.div(d, 2), nz)
    y = lax.div(d, 2 * nz)
    zh = lax.rem(b, nh)
    x = lax.div(b, nh)

    def dev(xx, yy, hz, lz, core):
        return ((yy * nz + lz) * 2 + core, xx * nh + hz)

    def copy(src, dst, send, recv, where):
        return pltpu.make_async_remote_copy(
            src_ref=src, dst_ref=dst, send_sem=send, recv_sem=recv,
            device_id=where, device_id_type=MESH,
        )

    mine_l = lax.div(zh, hh) == c

    barrier = pltpu.get_barrier_semaphore()

    def greet(where):
        pl.semaphore_signal(barrier, inc=1, device_id=where, device_id_type=MESH)

    left = (lax.rem(d + domains - 1, domains), b)
    right = (lax.rem(d + 1, domains), b)
    greet(left)
    greet(right)
    for h in range(hh):
        for s in range(2):
            src_h = c * hh + h
            pl.when(jnp.logical_not((src_h == zh) & (c == s)))(
                functools.partial(greet, dev(x, y, src_h, zl, s)))
    for xx in range(nx):
        for s in range(2):
            pl.when(jnp.logical_not((x == xx) & (c == s)))(
                functools.partial(greet, dev(xx, y, zh, zl, s)))
    for yy in range(ny):
        pl.when(jnp.logical_not((x == y) & (y == yy)))(
            functools.partial(greet, dev(y, yy, zh, zl, c)))
    half = lax.div(zl, nz // 2)
    for lz in range(nz):
        pl.when(jnp.logical_not((zl == lz) & (c == half)))(
            functools.partial(greet, dev(x, y, zh, lz, half)))

    for cell in range(cells):
        live = cell < cnt_ref[0]
        cols = slice(cell * npc, (cell + 1) * npc)
        rt = tile_of(ext, 128)
        for r in range(ext // rt):
            ids = lax.broadcasted_iota(jnp.int32, (rt, npc), 0) + r * rt
            hit = (conn_ref[cell:cell + 1, :] == ids) & live
            st[r * rt:(r + 1) * rt, cols] = jnp.where(hit, 1.0, 0.0).astype(jnp.bfloat16)

    rt = tile_of(npc, 256)
    ct = tile_of(ext, 256)
    for cell in range(cells):
        def gather_cols(i, carry, cell=cell):
            r = pl.multiple_of(lax.div(i, ext // ct) * rt, rt)
            e = pl.multiple_of(lax.rem(i, ext // ct) * ct, ct)
            t = lax.dot_general(
                h_ref[cell, pl.ds(r, rt), :], st[pl.ds(e, ct), cell * npc:(cell + 1) * npc],
                (((1,), (1,)), ((), ())), preferred_element_type=jnp.float32)
            hi = t.astype(jnp.bfloat16)
            thi[pl.ds(cell * npc + r, rt), pl.ds(e, ct)] = hi
            tlo[pl.ds(cell * npc + r, rt), pl.ds(e, ct)] = (t - hi.astype(jnp.float32)).astype(jnp.bfloat16)
            return carry
        lax.fori_loop(0, (npc // rt) * (ext // ct), gather_cols, 0)

    art = tile_of(ext, 256)

    def scatter_rows(i, carry):
        r = pl.multiple_of(lax.div(i, ext // ct) * art, art)
        e = pl.multiple_of(lax.rem(i, ext // ct) * ct, ct)
        rows = st[pl.ds(r, art), :]
        a = jnp.dot(rows, thi[:, pl.ds(e, ct)], preferred_element_type=jnp.float32)
        a += jnp.dot(rows, tlo[:, pl.ds(e, ct)], preferred_element_type=jnp.float32)
        hi = a.astype(jnp.bfloat16)
        ahi[pl.ds(r, art), pl.ds(e, ct)] = hi
        alo[pl.ds(r, art), pl.ds(e, ct)] = (a - hi.astype(jnp.float32)).astype(jnp.bfloat16)
        return carry
    lax.fori_loop(0, (ext // art) * (ext // ct), scatter_rows, 0)

    def column(row):
        return jnp.transpose(jnp.broadcast_to(row, (row.shape[1], row.shape[1])))[:, :1]

    def spread(row):
        return jnp.broadcast_to(column(row), (ghost, width))

    for i in range(4):
        mext[ghost * (i + 1):ghost * (i + 2), :] = spread(im_ref[i:i + 1, :])
    vext[ghost:ghost + own, :] = w_ref[...]

    as_int = lambda flag: flag.astype(jnp.int32)
    total = (2 + (nh - as_int(mine_l)) + (2 * nx - 1) + (nx - as_int(x == y))
             + (nz - as_int(half == c)))
    pl.semaphore_wait(barrier, total)

    first = []
    for side, where in ((0, left), (1, right)):
        other = 1 - side
        rows = slice(0, ghost) if side == 0 else slice(own - ghost, own)
        land = slice(own + ghost, ext) if side == 0 else slice(0, ghost)
        first.append(copy(im_ref, imx.at[other], s_im.at[side], r_im.at[other], where))
        first.append(copy(w_ref.at[rows], vext.at[land], s_w.at[side], r_w.at[other], where))
    for one in first:
        one.start()
    for one in first:
        one.wait_recv()
    mext[0:ghost, :] = spread(imx[0, 3:4, :])
    mext[own + ghost:ext, :] = spread(imx[1, 0:1, :])
    ys[0] = vext[...].astype(jnp.float32)

    def side_of(which):
        return c if which == 0 else 1 - c

    def u_send(k, which):
        s = side_of(which)
        where = (lax.rem(d + domains + 2 * s - 1, domains), b)
        if k < DEGREE - 1:
            src, dst = us.at[k, s], ur.at[k, 1 - s]
        else:
            out = pl.ds(pl.multiple_of(s * ghost, ghost), ghost)
            src, dst = us.at[k, s, out], ur.at[k, 1 - s, out]
        return copy(src, dst, s_u.at[k, s], r_u.at[k, 1 - s], where)

    def u_recv(k, which):
        s = side_of(which)
        where = (lax.rem(d + domains + 2 * s - 1, domains), b)
        got = ur.at[k, s]
        if k == DEGREE - 1:
            got = ur.at[k, s, pl.ds(pl.multiple_of((1 - s) * ghost, ghost), ghost)]
        return copy(got, got, s_u.at[k, s], r_u.at[k, s], where)

    def product(rows):
        v = vext[...]
        return (jnp.dot(ahi[rows, :], v, preferred_element_type=jnp.float32)
                + jnp.dot(alo[rows, :], v, preferred_element_type=jnp.float32))

    def advance(k, rows, summed):
        cur, old = k % 2, 1 - k % 2
        av = mext[rows, :] * summed
        now = ys[cur, rows, :]
        if k == 0:
            new = (av - CENTER * now) * (1.0 / HALFWIDTH)
        else:
            new = (2.0 / HALFWIDTH) * (av - CENTER * now) - ys[old, rows, :]
        if k < DEGREE - 1:
            ys[old, rows, :] = new
        return new.astype(jnp.bfloat16)

    def place(own_row, n, value):
        rows = pl.ds(own_row, n)
        rb[x, c, rows, :] = value
        filt_ref[rows, :] = value

        @pl.when(mine_l)
        def _():
            lb[lax.rem(zh, hh), c, rows, :] = value

    piece = ((1, 3 * ghost), (3, ghost))

    def piece_rows(s, p):
        off = (1 - s) * ghost if p == 0 else s * 3 * ghost
        n = piece[p][1]
        if isinstance(off, int):
            return pl.ds(off, n)
        return pl.ds(pl.multiple_of(off, ghost), n)

    def r_send(xx, s, p):
        rows = piece_rows(c, p)
        ref = rb.at[x, c, rows]
        return copy(ref, ref, s_r.at[xx, s, p], r_r.at[x, c, p], dev(xx, y, zh, zl, s))

    def r_recv(xx, s, p):
        ref = rb.at[xx, s, piece_rows(s, p)]
        return copy(ref, ref, s_r.at[xx, s, p], r_r.at[xx, s, p], dev(xx, y, zh, zl, s))

    def l_send(hz, p):
        rows = piece_rows(c, p)
        return copy(rb.at[x, c, rows], lb.at[lax.rem(zh, hh), c, rows], s_l.at[hz, p],
                    r_l.at[lax.rem(zh, hh), c, p], dev(x, y, hz, zl, lax.div(zh, hh)))

    def l_recv(h, s, p):
        ref = lb.at[h, s, piece_rows(s, p)]
        return copy(ref, ref, s_l.at[h, p], r_l.at[h, s, p], dev(x, y, c * hh + h, zl, s))

    def not_self_r(xx, s):
        return jnp.logical_not((x == xx) & (c == s))

    def not_self_l(hz):
        return jnp.logical_not((zh == hz) & mine_l)

    def not_self_lr(h, s):
        return jnp.logical_not((zh == c * hh + h) & (c == s))

    def send_piece(p):
        for hz in range(nh):
            pl.when(not_self_l(hz))(lambda hz=hz: l_send(hz, p).start())
        for xx in range(nx):
            for s in range(2):
                pl.when(not_self_r(xx, s))(lambda xx=xx, s=s: r_send(xx, s, p).start())

    for k in range(DEGREE):
        last = k == DEGREE - 1
        offs = []
        for which in range(2):
            s = side_of(which)
            off = pl.multiple_of(s * own, block)
            offs.append((s, off))
            u = product(pl.ds(off, block))
            us_f[pl.ds(off, block), :] = u
            us[k, s] = u.astype(us.dtype)
            u_send(k, which).start()
        mid = slice(block, own)
        mid_new = advance(k, mid, product(mid))
        if last:
            place(ghost, own - block, mid_new)
        fresh = []
        for which in (1, 0):
            s, off = offs[which]
            u_recv(k, which).wait_recv()
            if not last:
                rows = pl.ds(off, block)
                fresh.append((rows, advance(
                    k, rows, us_f[rows, :] + ur[k, s].astype(jnp.float32))))
            else:
                inner = pl.multiple_of((1 - s) * ghost, ghost)
                rows = pl.ds(pl.multiple_of(off + inner, ghost), ghost)
                new = advance(
                    k, rows,
                    us_f[rows, :] + ur[k, s, pl.ds(inner, ghost), :].astype(jnp.float32))
                place(pl.multiple_of(s * 3 * ghost, ghost), ghost, new)
                send_piece(1 - which)
        if not last:
            vext[mid, :] = mid_new
            for rows, value in fresh:
                vext[rows, :] = value

    for p in range(2):
        for xx in range(nx):
            for s in range(2):
                pl.when(not_self_r(xx, s))(lambda xx=xx, s=s: r_recv(xx, s, p).wait_recv())
        for h in range(hh):
            for s in range(2):
                pl.when(not_self_lr(h, s))(lambda h=h, s=s: l_recv(h, s, p).wait_recv())
        for s in range(2):
            rows = piece_rows(s, p)
            right_op = jnp.concatenate([rb[xx, s, rows, :] for xx in range(nx)], axis=1)
            for h in range(hh):
                part = lax.dot_general(
                    lb[h, s, rows, :], right_op, (((0,), (0,)), ((), ())),
                    preferred_element_type=jnp.float32)
                hrows = slice(h * width, (h + 1) * width)
                if p == 0 and s == 0:
                    pacc[hrows, :] = part
                else:
                    pacc[hrows, :] += part

    def e_send(xx):
        return copy(es.at[xx], er.at[y], s_e.at[xx], r_e.at[y], dev(xx, x, zh, zl, c))

    def e_recv(yy):
        return copy(er.at[yy], er.at[yy], s_e.at[yy], r_e.at[yy], dev(y, yy, zh, zl, c))

    for xx in range(nx):
        value = pacc[:, xx * width:(xx + 1) * width].astype(es.dtype)
        away = jnp.logical_not((x == xx) & (x == y))

        @pl.when(away)
        def _(xx=xx, value=value):
            es[xx] = value
            e_send(xx).start()

        @pl.when(jnp.logical_not(away))
        def _(value=value):
            er[y] = value
    acc = None
    for yy in range(ny):
        pl.when(jnp.logical_not((x == y) & (y == yy)))(lambda yy=yy: e_recv(yy).wait_recv())
        term = er[yy].astype(jnp.float32)
        acc = term if acc is None else acc + term
    zs[...] = acc.astype(zs.dtype)

    targets = 2 * (nz // 2)

    def z_target(j):
        return c * (nz // 2) + j // 2, j % 2

    def z_away(j):
        lz, core = z_target(j)
        return jnp.logical_not((zl == lz) & (c == core))

    def z_send(j):
        lz, core = z_target(j)
        return copy(zs.at[j * out_rows:(j + 1) * out_rows], zr.at[zl], s_z.at[j], r_z.at[zl],
                    dev(x, y, zh, lz, core))

    def z_recv(lz):
        return copy(zr.at[lz], zr.at[lz], s_z.at[lz], r_z.at[lz], dev(x, y, zh, lz, half))

    for j in range(targets):
        pl.when(z_away(j))(lambda j=j: z_send(j).start())

        @pl.when(jnp.logical_not(z_away(j)))
        def _(j=j):
            zr[zl] = zs[j * out_rows:(j + 1) * out_rows, :]
    acc = None
    for lz in range(nz):
        pl.when(jnp.logical_not((zl == lz) & (c == half)))(lambda lz=lz: z_recv(lz).wait_recv())
        term = zr[lz].astype(jnp.float32)
        acc = term if acc is None else acc + term
    marg_ref[...] = acc * (1.0 / float(own * domains) ** 0.5)

    for one in first:
        one.wait_send()
    for k in range(DEGREE):
        for which in range(2):
            u_send(k, which).wait_send()
    for p in range(2):
        for hz in range(nh):
            pl.when(not_self_l(hz))(lambda hz=hz, p=p: l_send(hz, p).wait_send())
        for xx in range(nx):
            for s in range(2):
                pl.when(not_self_r(xx, s))(lambda xx=xx, s=s, p=p: r_send(xx, s, p).wait_send())
    for xx in range(nx):
        pl.when(jnp.logical_not((x == xx) & (x == y)))(lambda xx=xx: e_send(xx).wait_send())
    for j in range(targets):
        pl.when(z_away(j))(lambda j=j: z_send(j).wait_send())


def local(shape, wavefunctions, cell_ham, connectivity, inv_mass, cell_count):
    nx, ny, nh, nz = shape
    own, width = wavefunctions.shape
    cells, npc, _ = cell_ham.shape
    ghost = own // 4
    ext = own + 2 * ghost
    block = 2 * ghost
    hh = nh // 2
    out_rows = width // 4
    bf, f32 = jnp.bfloat16, jnp.float32
    sent = f32
    dma = pltpu.SemaphoreType.DMA
    vm = pl.BlockSpec(memory_space=pltpu.VMEM)
    filtered, rows = pl.pallas_call(
        functools.partial(kernel, shape),
        out_shape=(jax.ShapeDtypeStruct((own, width), bf), jax.ShapeDtypeStruct((out_rows, width), f32)),
        in_specs=[vm, vm, vm, vm, pl.BlockSpec(memory_space=pltpu.SMEM)],
        out_specs=(vm, vm),
        scratch_shapes=[
            pltpu.VMEM((ext, cells * npc), bf),
            pltpu.VMEM((cells * npc, ext), bf),
            pltpu.VMEM((cells * npc, ext), bf),
            pltpu.VMEM((ext, ext), bf),
            pltpu.VMEM((ext, ext), bf),
            pltpu.VMEM((ext, width), f32),
            pltpu.VMEM((2, 4, ghost), f32),
            pltpu.VMEM((ext, width), bf),
            pltpu.VMEM((2, ext, width), f32),
            pltpu.VMEM((ext, width), f32),
            pltpu.VMEM((DEGREE, 2, block, width), sent),
            pltpu.VMEM((DEGREE, 2, block, width), sent),
            pltpu.VMEM((nx, 2, own, width), bf),
            pltpu.VMEM((hh, 2, own, width), bf),
            pltpu.VMEM((hh * width, nx * width), f32),
            pltpu.VMEM((nx, hh * width, width), bf),
            pltpu.VMEM((ny, hh * width, width), bf),
            pltpu.VMEM((hh * width, width), bf),
            pltpu.VMEM((nz, out_rows, width), bf),
            dma((2,)), dma((2,)), dma((2,)), dma((2,)),
            dma((DEGREE, 2)), dma((DEGREE, 2)),
            dma((nx, 2, 2)), dma((nx, 2, 2)),
            dma((nh, 2)), dma((hh, 2, 2)),
            dma((nx,)), dma((ny,)),
            dma((nz,)), dma((nz,)),
        ],
        compiler_params=pltpu.CompilerParams(
            collective_id=0, has_side_effects=True, vmem_limit_bytes=48 * 1024 * 1024),
        name="filter_margin",
    )(wavefunctions, cell_ham, connectivity, inv_mass.reshape(4, ghost), cell_count)
    return filtered, rows.T


def solution(mesh, shape=(NX, NY, NH, NZ)):
    return jax.shard_map(
        functools.partial(local, shape), mesh=mesh,
        in_specs=(P("dom", "band"), P("dom", None, None), P("dom", None), P("dom"), P("dom")),
        out_specs=(P("dom", "band"), P("band", "dom")),
        check_vma=False,
    )
```

```python
import functools

import jax
import jax.numpy as jnp
from jax import lax
from jax.experimental import pallas as pl
from jax.experimental.pallas import tpu as pltpu
from jax.sharding import PartitionSpec as P

DEGREE = 4
CENTER = 0.5
HALFWIDTH = 3.0
NX, NY, NH, NZ = 4, 4, 4, 8
MESH = pl.DeviceIdType.MESH


def tile_of(size, most):
    return most if size % most == 0 else size


def kernel(
    shape, w_ref, h_ref, conn_ref, im_ref, cnt_ref, filt_ref, marg_ref,
    st, thi, tlo, ahi, alo, mext, imx, vext, ys, us_f, us, ur, rb, lb, pacc, px,
    es, er, zs, zr,
    s_w, r_w, s_im, r_im, s_u, r_u, s_r, r_r, s_l, r_l, s_p, r_p, s_e, r_e, s_z, r_z,
):
    nx, ny, nh, nz = shape
    own, width = w_ref.shape
    cells, npc, _ = h_ref.shape
    ghost = own // 4
    ext = own + 2 * ghost
    block = 2 * ghost
    hh = nh // 2
    out_rows = width // 4
    domains = ny * nz * 2

    d = lax.axis_index("dom")
    b = lax.axis_index("band")
    c = lax.rem(d, 2)
    zl = lax.rem(lax.div(d, 2), nz)
    y = lax.div(d, 2 * nz)
    zh = lax.rem(b, nh)
    x = lax.div(b, nh)

    def dev(xx, yy, hz, lz, core):
        return ((yy * nz + lz) * 2 + core, xx * nh + hz)

    def copy(src, dst, send, recv, where):
        return pltpu.make_async_remote_copy(
            src_ref=src, dst_ref=dst, send_sem=send, recv_sem=recv,
            device_id=where, device_id_type=MESH,
        )

    ring = {"h": (zh, nh), "x": (x, nx)}

    def at(axis, step):
        place, count = ring[axis]
        return lax.rem(place + count + step, count)

    def beside(axis, step):
        if axis == "h":
            return dev(x, y, at("h", step), zl, c)
        return dev(at("x", step), y, zh, zl, c)

    barrier = pltpu.get_barrier_semaphore()

    def greet(where):
        pl.semaphore_signal(barrier, inc=1, device_id=where, device_id_type=MESH)

    left = (lax.rem(d + domains - 1, domains), b)
    right = (lax.rem(d + 1, domains), b)
    greet(left)
    greet(right)
    greet(beside("h", 1))
    greet(beside("h", -1))
    if nx > 1:
        greet(beside("x", 1))
        greet(beside("x", -1))
    partner = dev(x, y, zh, zl, 1 - c)
    greet(partner)
    for yy in range(ny):
        pl.when(jnp.logical_not((x == y) & (y == yy)))(
            functools.partial(greet, dev(y, yy, zh, zl, c)))
    half = lax.div(zl, nz // 2)
    for lz in range(nz):
        pl.when(jnp.logical_not((zl == lz) & (c == half)))(
            functools.partial(greet, dev(x, y, zh, lz, half)))

    for cell in range(cells):
        live = cell < cnt_ref[0]
        cols = slice(cell * npc, (cell + 1) * npc)
        rt = tile_of(ext, 128)
        for r in range(ext // rt):
            ids = lax.broadcasted_iota(jnp.int32, (rt, npc), 0) + r * rt
            hit = (conn_ref[cell:cell + 1, :] == ids) & live
            st[r * rt:(r + 1) * rt, cols] = jnp.where(hit, 1.0, 0.0).astype(jnp.bfloat16)

    rt = tile_of(npc, 256)
    ct = tile_of(ext, 256)
    for cell in range(cells):
        def gather_cols(i, carry, cell=cell):
            r = pl.multiple_of(lax.div(i, ext // ct) * rt, rt)
            e = pl.multiple_of(lax.rem(i, ext // ct) * ct, ct)
            t = lax.dot_general(
                h_ref[cell, pl.ds(r, rt), :], st[pl.ds(e, ct), cell * npc:(cell + 1) * npc],
                (((1,), (1,)), ((), ())), preferred_element_type=jnp.float32)
            hi = t.astype(jnp.bfloat16)
            thi[pl.ds(cell * npc + r, rt), pl.ds(e, ct)] = hi
            tlo[pl.ds(cell * npc + r, rt), pl.ds(e, ct)] = (t - hi.astype(jnp.float32)).astype(jnp.bfloat16)
            return carry
        lax.fori_loop(0, (npc // rt) * (ext // ct), gather_cols, 0)

    art = tile_of(ext, 256)

    def scatter_rows(i, carry):
        r = pl.multiple_of(lax.div(i, ext // ct) * art, art)
        e = pl.multiple_of(lax.rem(i, ext // ct) * ct, ct)
        rows = st[pl.ds(r, art), :]
        a = jnp.dot(rows, thi[:, pl.ds(e, ct)], preferred_element_type=jnp.float32)
        a += jnp.dot(rows, tlo[:, pl.ds(e, ct)], preferred_element_type=jnp.float32)
        hi = a.astype(jnp.bfloat16)
        ahi[pl.ds(r, art), pl.ds(e, ct)] = hi
        alo[pl.ds(r, art), pl.ds(e, ct)] = (a - hi.astype(jnp.float32)).astype(jnp.bfloat16)
        return carry
    lax.fori_loop(0, (ext // art) * (ext // ct), scatter_rows, 0)

    def column(row):
        return jnp.transpose(jnp.broadcast_to(row, (row.shape[1], row.shape[1])))[:, :1]

    def spread(row):
        return jnp.broadcast_to(column(row), (ghost, width))

    for i in range(4):
        mext[ghost * (i + 1):ghost * (i + 2), :] = spread(im_ref[i:i + 1, :])
    vext[ghost:ghost + own, :] = w_ref[...]

    as_int = lambda flag: flag.astype(jnp.int32)
    total = (2 + 2 + (2 if nx > 1 else 0) + 1 + (nx - as_int(x == y))
             + (nz - as_int(half == c)))
    pl.semaphore_wait(barrier, total)

    first = []
    for side, where in ((0, left), (1, right)):
        other = 1 - side
        rows = slice(0, ghost) if side == 0 else slice(own - ghost, own)
        land = slice(own + ghost, ext) if side == 0 else slice(0, ghost)
        first.append(copy(im_ref, imx.at[other], s_im.at[side], r_im.at[other], where))
        first.append(copy(w_ref.at[rows], vext.at[land], s_w.at[side], r_w.at[other], where))
    for one in first:
        one.start()
    for one in first:
        one.wait_recv()
    mext[0:ghost, :] = spread(imx[0, 3:4, :])
    mext[own + ghost:ext, :] = spread(imx[1, 0:1, :])
    ys[0] = vext[...].astype(jnp.float32)

    def side_of(which):
        return c if which == 0 else 1 - c

    def u_send(k, which):
        s = side_of(which)
        where = (lax.rem(d + domains + 2 * s - 1, domains), b)
        if k < DEGREE - 1:
            src, dst = us.at[k, s], ur.at[k, 1 - s]
        else:
            out = pl.ds(pl.multiple_of(s * ghost, ghost), ghost)
            src, dst = us.at[k, s, out], ur.at[k, 1 - s, out]
        return copy(src, dst, s_u.at[k, s], r_u.at[k, 1 - s], where)

    def u_recv(k, which):
        s = side_of(which)
        where = (lax.rem(d + domains + 2 * s - 1, domains), b)
        got = ur.at[k, s]
        if k == DEGREE - 1:
            got = ur.at[k, s, pl.ds(pl.multiple_of((1 - s) * ghost, ghost), ghost)]
        return copy(got, got, s_u.at[k, s], r_u.at[k, s], where)

    def product(rows):
        v = vext[...]
        return (jnp.dot(ahi[rows, :], v, preferred_element_type=jnp.float32)
                + jnp.dot(alo[rows, :], v, preferred_element_type=jnp.float32))

    def advance(k, rows, summed):
        cur, old = k % 2, 1 - k % 2
        av = mext[rows, :] * summed
        now = ys[cur, rows, :]
        if k == 0:
            new = (av - CENTER * now) * (1.0 / HALFWIDTH)
        else:
            new = (2.0 / HALFWIDTH) * (av - CENTER * now) - ys[old, rows, :]
        if k < DEGREE - 1:
            ys[old, rows, :] = new
        return new.astype(jnp.bfloat16)

    def place(own_row, n, value):
        rows = pl.ds(own_row, n)
        lb[zh, rows, :] = value
        rb[x, rows, :] = value
        filt_ref[rows, :] = value

    def piece_rows(core, p):
        if p == 0:
            return pl.ds(pl.multiple_of((1 - core) * ghost, ghost), 3 * ghost)
        return pl.ds(pl.multiple_of(core * 3 * ghost, ghost), ghost)

    bufs = {"h": (lb, s_l, r_l), "x": (rb, s_r, r_r)}
    toward = 2 * c - 1

    def block_send(axis, i, p):
        buf, send, recv = bufs[axis]
        step = (1, -1, -toward)[i]
        slot = ring[axis][0] if i < 2 else at(axis, toward)
        ref = buf.at[slot, piece_rows(c, p)]
        return copy(ref, ref, send.at[i, p], recv.at[i, p], beside(axis, step))

    def block_recv(axis, i, p):
        buf, send, recv = bufs[axis]
        slot = at(axis, (-1, 1, 2)[i])
        step = (-1, 1, toward)[i]
        ref = buf.at[slot, piece_rows(c, p)]
        return copy(ref, ref, send.at[i, p], recv.at[i, p], beside(axis, step))

    axes = ("h", "x") if nx > 1 else ("h",)

    def send_piece(p):
        for axis in axes:
            for i in range(2):
                block_send(axis, i, p).start()

    def pass_on(axis, p):
        for i in range(2):
            block_recv(axis, i, p).wait_recv()
        block_send(axis, 2, p).start()

    for k in range(DEGREE):
        last = k == DEGREE - 1
        offs = []
        for which in range(2):
            s = side_of(which)
            off = pl.multiple_of(s * own, block)
            offs.append((s, off))
            u = product(pl.ds(off, block))
            us_f[pl.ds(off, block), :] = u
            us[k, s] = u.astype(us.dtype)
            u_send(k, which).start()
        mid = slice(block, own)
        mid_new = advance(k, mid, product(mid))
        if last:
            place(ghost, own - block, mid_new)
        fresh = []
        for which in (1, 0):
            s, off = offs[which]
            u_recv(k, which).wait_recv()
            if not last:
                rows = pl.ds(off, block)
                fresh.append((rows, advance(
                    k, rows, us_f[rows, :] + ur[k, s].astype(jnp.float32))))
            else:
                inner = pl.multiple_of((1 - s) * ghost, ghost)
                rows = pl.ds(pl.multiple_of(off + inner, ghost), ghost)
                new = advance(
                    k, rows,
                    us_f[rows, :] + ur[k, s, pl.ds(inner, ghost), :].astype(jnp.float32))
                place(pl.multiple_of(s * 3 * ghost, ghost), ghost, new)
                send_piece(1 - which)
        if not last:
            vext[mid, :] = mid_new
            for rows, value in fresh:
                vext[rows, :] = value

    for p in range(2):
        for axis in reversed(axes):
            pass_on(axis, p)
    if nx > 1:
        for p in range(2):
            block_recv("x", 2, p).wait_recv()
    right_op = jnp.concatenate([rb[xx] for xx in range(nx)], axis=1)

    def p_rows(o):
        return pl.ds(pl.multiple_of(o * width, width), width)

    def p_send(o):
        h = lax.rem(o, hh)
        return copy(pacc.at[p_rows(o)], px.at[h], s_p.at[h], r_p.at[h], partner)

    def p_recv(h):
        return copy(px.at[h], px.at[h], s_p.at[h], r_p.at[h], partner)

    for step in (0, -1, 1, 2):
        o = at("h", step)
        if step == 2:
            for p in range(2):
                block_recv("h", 2, p).wait_recv()
        pacc[p_rows(o), :] = lax.dot_general(
            lb[o], right_op, (((0,), (0,)), ((), ())), preferred_element_type=jnp.float32)
        pl.when(lax.div(o, hh) != c)(lambda o=o: p_send(o).start())
    for h in range(hh):
        p_recv(h).wait_recv()

    def e_send(xx):
        return copy(es.at[xx], er.at[y], s_e.at[xx], r_e.at[y], dev(xx, x, zh, zl, c))

    def e_recv(yy):
        return copy(er.at[yy], er.at[yy], s_e.at[yy], r_e.at[yy], dev(y, yy, zh, zl, c))

    sums = [pacc[p_rows(c * hh + h), :] + px[h] for h in range(hh)]
    for xx in range(nx):
        cols = slice(xx * width, (xx + 1) * width)
        value = jnp.concatenate([one[:, cols] for one in sums], axis=0).astype(es.dtype)
        away = jnp.logical_not((x == xx) & (x == y))

        @pl.when(away)
        def _(xx=xx, value=value):
            es[xx] = value
            e_send(xx).start()

        @pl.when(jnp.logical_not(away))
        def _(value=value):
            er[y] = value
    acc = None
    for yy in range(ny):
        pl.when(jnp.logical_not((x == y) & (y == yy)))(lambda yy=yy: e_recv(yy).wait_recv())
        term = er[yy].astype(jnp.float32)
        acc = term if acc is None else acc + term
    zs[...] = acc.astype(zs.dtype)

    targets = 2 * (nz // 2)

    def z_target(j):
        return c * (nz // 2) + j // 2, j % 2

    def z_away(j):
        lz, core = z_target(j)
        return jnp.logical_not((zl == lz) & (c == core))

    def z_send(j):
        lz, core = z_target(j)
        return copy(zs.at[j * out_rows:(j + 1) * out_rows], zr.at[zl], s_z.at[j], r_z.at[zl],
                    dev(x, y, zh, lz, core))

    def z_recv(lz):
        return copy(zr.at[lz], zr.at[lz], s_z.at[lz], r_z.at[lz], dev(x, y, zh, lz, half))

    for j in range(targets):
        pl.when(z_away(j))(lambda j=j: z_send(j).start())

        @pl.when(jnp.logical_not(z_away(j)))
        def _(j=j):
            zr[zl] = zs[j * out_rows:(j + 1) * out_rows, :]
    acc = None
    for lz in range(nz):
        pl.when(jnp.logical_not((zl == lz) & (c == half)))(lambda lz=lz: z_recv(lz).wait_recv())
        term = zr[lz].astype(jnp.float32)
        acc = term if acc is None else acc + term
    marg_ref[...] = acc * (1.0 / float(own * domains) ** 0.5)

    for one in first:
        one.wait_send()
    for k in range(DEGREE):
        for which in range(2):
            u_send(k, which).wait_send()
    for p in range(2):
        for axis in axes:
            for i in range(3):
                block_send(axis, i, p).wait_send()
    for h in range(hh):
        p_send((1 - c) * hh + h).wait_send()
    for xx in range(nx):
        pl.when(jnp.logical_not((x == xx) & (x == y)))(lambda xx=xx: e_send(xx).wait_send())
    for j in range(targets):
        pl.when(z_away(j))(lambda j=j: z_send(j).wait_send())


def local(shape, wavefunctions, cell_ham, connectivity, inv_mass, cell_count):
    nx, ny, nh, nz = shape
    own, width = wavefunctions.shape
    cells, npc, _ = cell_ham.shape
    ghost = own // 4
    ext = own + 2 * ghost
    block = 2 * ghost
    hh = nh // 2
    out_rows = width // 4
    bf, f32 = jnp.bfloat16, jnp.float32
    sent = f32
    dma = pltpu.SemaphoreType.DMA
    vm = pl.BlockSpec(memory_space=pltpu.VMEM)
    filtered, rows = pl.pallas_call(
        functools.partial(kernel, shape),
        out_shape=(jax.ShapeDtypeStruct((own, width), bf), jax.ShapeDtypeStruct((out_rows, width), f32)),
        in_specs=[vm, vm, vm, vm, pl.BlockSpec(memory_space=pltpu.SMEM)],
        out_specs=(vm, vm),
        scratch_shapes=[
            pltpu.VMEM((ext, cells * npc), bf),
            pltpu.VMEM((cells * npc, ext), bf),
            pltpu.VMEM((cells * npc, ext), bf),
            pltpu.VMEM((ext, ext), bf),
            pltpu.VMEM((ext, ext), bf),
            pltpu.VMEM((ext, width), f32),
            pltpu.VMEM((2, 4, ghost), f32),
            pltpu.VMEM((ext, width), bf),
            pltpu.VMEM((2, ext, width), f32),
            pltpu.VMEM((ext, width), f32),
            pltpu.VMEM((DEGREE, 2, block, width), sent),
            pltpu.VMEM((DEGREE, 2, block, width), sent),
            pltpu.VMEM((nx, own, width), bf),
            pltpu.VMEM((nh, own, width), bf),
            pltpu.VMEM((nh * width, nx * width), f32),
            pltpu.VMEM((hh, width, nx * width), f32),
            pltpu.VMEM((nx, hh * width, width), bf),
            pltpu.VMEM((ny, hh * width, width), bf),
            pltpu.VMEM((hh * width, width), bf),
            pltpu.VMEM((nz, out_rows, width), bf),
            dma((2,)), dma((2,)), dma((2,)), dma((2,)),
            dma((DEGREE, 2)), dma((DEGREE, 2)),
            dma((3, 2)), dma((3, 2)), dma((3, 2)), dma((3, 2)),
            dma((hh,)), dma((hh,)),
            dma((nx,)), dma((ny,)),
            dma((nz,)), dma((nz,)),
        ],
        compiler_params=pltpu.CompilerParams(
            collective_id=0, has_side_effects=True, vmem_limit_bytes=48 * 1024 * 1024),
        name="filter_margin",
    )(wavefunctions, cell_ham, connectivity, inv_mass.reshape(4, ghost), cell_count)
    return filtered, rows.T


def solution(mesh, shape=(NX, NY, NH, NZ)):
    return jax.shard_map(
        functools.partial(local, shape), mesh=mesh,
        in_specs=(P("dom", "band"), P("dom", None, None), P("dom", None), P("dom"), P("dom")),
        out_specs=(P("dom", "band"), P("band", "dom")),
        check_vma=False,
    )
```

```python
import functools

import jax
import jax.numpy as jnp
from jax import lax
from jax.experimental import pallas as pl
from jax.experimental.pallas import tpu as pltpu
from jax.sharding import PartitionSpec as P

DEGREE = 4
CENTER = 0.5
HALFWIDTH = 3.0
NX, NY, NH, NZ = 4, 4, 4, 8
MESH = pl.DeviceIdType.MESH


def tile_of(size, most):
    return most if size % most == 0 else size


def kernel(
    shape, w_hbm, h_hbm, conn_hbm, im_hbm, cnt_ref, filt_ref, marg_ref,
    h_ref, conn_ref, im_ref, s_in,
    st, thi, tlo, ahi, alo, mext, imx, vext, ys, us_f, us, ur, rb, lb, pp, px, pb,
    esa, era, esb, erb, esm, erm, ms, mr, zs, zr,
    s_w, r_w, s_im, r_im, s_u, r_u, s_r, r_r, s_l, r_l, s_p, r_p, s_ea, r_ea, s_eb, r_eb, s_em, r_em, s_m, r_m, s_z, r_z,
):
    nx, ny, nh, nz = shape
    own, width = w_hbm.shape
    cells, npc, _ = h_ref.shape
    ghost = own // 4
    ext = own + 2 * ghost
    block = 2 * ghost
    out_rows = width // 4
    domains = ny * nz * 2

    d = lax.axis_index("dom")
    b = lax.axis_index("band")
    c = lax.rem(d, 2)
    zl = lax.rem(lax.div(d, 2), nz)
    y = lax.div(d, 2 * nz)
    zh = lax.rem(b, nh)
    x = lax.div(b, nh)

    def dev(xx, yy, hz, lz, core):
        return ((yy * nz + lz) * 2 + core, xx * nh + hz)

    def copy(src, dst, send, recv, where):
        return pltpu.make_async_remote_copy(
            src_ref=src, dst_ref=dst, send_sem=send, recv_sem=recv,
            device_id=where, device_id_type=MESH,
        )

    ring = {"h": (zh, nh), "x": (x, nx)}

    def at(axis, step):
        place, count = ring[axis]
        return lax.rem(place + count + step, count)

    def beside(axis, step):
        if axis == "h":
            return dev(x, y, at("h", step), zl, c)
        return dev(at("x", step), y, zh, zl, c)

    loads = [
        pltpu.make_async_copy(w_hbm, vext.at[slice(ghost, ghost + own)], s_in.at[0]),
        pltpu.make_async_copy(im_hbm, im_ref, s_in.at[1]),
        pltpu.make_async_copy(conn_hbm, conn_ref, s_in.at[2]),
        pltpu.make_async_copy(h_hbm, h_ref, s_in.at[3]),
    ]
    for one in loads:
        one.start()

    toward = 2 * c - 1
    mirror = dev(x, y, at("h", toward), zl, 1 - c)

    barrier = pltpu.get_barrier_semaphore()

    def greet(where):
        pl.semaphore_signal(barrier, inc=1, device_id=where, device_id_type=MESH)

    left = (lax.rem(d + domains - 1, domains), b)
    right = (lax.rem(d + 1, domains), b)
    greet(left)
    greet(right)
    greet(beside("h", toward))
    greet(mirror)
    if nx > 1:
        greet(beside("x", 1))
        greet(beside("x", -1))
    partner = dev(x, y, zh, zl, 1 - c)
    greet(partner)
    for yy in range(ny):
        pl.when(jnp.logical_not((x == y) & (y == yy)))(
            functools.partial(greet, dev(y, yy, zh, zl, c)))
    for yy in range(ny):
        pl.when(y != yy)(functools.partial(greet, dev(x, yy, zh, zl, c)))
    ahead = lax.rem(lax.div(zl, 2) + nh - zh, nh)
    half = jnp.where((ahead == 1) | (ahead == 2), 1, 0)
    for lz in range(nz):
        pl.when(jnp.logical_not((zl == lz) & (c == half)))(
            functools.partial(greet, dev(x, y, zh, lz, half)))

    loads[0].wait()
    loads[1].wait()
    as_int = lambda flag: flag.astype(jnp.int32)
    total = (2 + 2 + (2 if nx > 1 else 0) + 1 + (nx - as_int(x == y)) + (ny - 1)
             + (nz - as_int(half == c)))
    pl.semaphore_wait(barrier, total)

    first = []
    for side, where in ((0, left), (1, right)):
        other = 1 - side
        rows = slice(ghost, 2 * ghost) if side == 0 else slice(own, own + ghost)
        land = slice(own + ghost, ext) if side == 0 else slice(0, ghost)
        first.append(copy(im_ref, imx.at[other], s_im.at[side], r_im.at[other], where))
        first.append(copy(vext.at[rows], vext.at[land], s_w.at[side], r_w.at[other], where))
    for one in first:
        one.start()
    for one in loads[2:]:
        one.wait()

    for cell in range(cells):
        live = cell < cnt_ref[0]
        cols = slice(cell * npc, (cell + 1) * npc)
        rt = tile_of(ext, 128)
        for r in range(ext // rt):
            ids = lax.broadcasted_iota(jnp.int32, (rt, npc), 0) + r * rt
            hit = (conn_ref[cell:cell + 1, :] == ids) & live
            st[r * rt:(r + 1) * rt, cols] = jnp.where(hit, 1.0, 0.0).astype(jnp.bfloat16)

    rt = tile_of(npc, 256)
    ct = tile_of(ext, 256)
    for cell in range(cells):
        def gather_cols(i, carry, cell=cell):
            r = pl.multiple_of(lax.div(i, ext // ct) * rt, rt)
            e = pl.multiple_of(lax.rem(i, ext // ct) * ct, ct)
            t = lax.dot_general(
                h_ref[cell, pl.ds(r, rt), :], st[pl.ds(e, ct), cell * npc:(cell + 1) * npc],
                (((1,), (1,)), ((), ())), preferred_element_type=jnp.float32)
            hi = t.astype(jnp.bfloat16)
            thi[pl.ds(cell * npc + r, rt), pl.ds(e, ct)] = hi
            tlo[pl.ds(cell * npc + r, rt), pl.ds(e, ct)] = (t - hi.astype(jnp.float32)).astype(jnp.bfloat16)
            return carry
        lax.fori_loop(0, (npc // rt) * (ext // ct), gather_cols, 0)

    art = tile_of(ext, 256)

    def scatter_rows(i, carry):
        r = pl.multiple_of(lax.div(i, ext // ct) * art, art)
        e = pl.multiple_of(lax.rem(i, ext // ct) * ct, ct)
        rows = st[pl.ds(r, art), :]
        a = jnp.dot(rows, thi[:, pl.ds(e, ct)], preferred_element_type=jnp.float32)
        a += jnp.dot(rows, tlo[:, pl.ds(e, ct)], preferred_element_type=jnp.float32)
        hi = a.astype(jnp.bfloat16)
        ahi[pl.ds(r, art), pl.ds(e, ct)] = hi
        alo[pl.ds(r, art), pl.ds(e, ct)] = (a - hi.astype(jnp.float32)).astype(jnp.bfloat16)
        return carry
    lax.fori_loop(0, (ext // art) * (ext // ct), scatter_rows, 0)

    def column(row):
        return jnp.transpose(jnp.broadcast_to(row, (row.shape[1], row.shape[1])))[:, :1]

    def spread(row):
        return jnp.broadcast_to(column(row), (ghost, width))

    for i in range(4):
        mext[ghost * (i + 1):ghost * (i + 2), :] = spread(im_ref[i:i + 1, :])
    for one in first:
        one.wait()
    mext[0:ghost, :] = spread(imx[0, 3:4, :])
    mext[own + ghost:ext, :] = spread(imx[1, 0:1, :])
    ys[0] = vext[...].astype(jnp.float32)

    def side_of(which):
        return c if which == 0 else 1 - c

    def u_send(k, which):
        s = side_of(which)
        where = (lax.rem(d + domains + 2 * s - 1, domains), b)
        if k < DEGREE - 1:
            src, dst = us.at[k, s], ur.at[k, 1 - s]
        else:
            out = pl.ds(pl.multiple_of(s * ghost, ghost), ghost)
            src, dst = us.at[k, s, out], ur.at[k, 1 - s, out]
        return copy(src, dst, s_u.at[k, s], r_u.at[k, 1 - s], where)

    def u_recv(k, which):
        s = side_of(which)
        where = (lax.rem(d + domains + 2 * s - 1, domains), b)
        got = ur.at[k, s]
        if k == DEGREE - 1:
            got = ur.at[k, s, pl.ds(pl.multiple_of((1 - s) * ghost, ghost), ghost)]
        return copy(got, got, s_u.at[k, s], r_u.at[k, s], where)

    def product(rows):
        v = vext[...]
        return (jnp.dot(ahi[rows, :], v, preferred_element_type=jnp.float32)
                + jnp.dot(alo[rows, :], v, preferred_element_type=jnp.float32))

    def advance(k, rows, summed):
        cur, old = k % 2, 1 - k % 2
        av = mext[rows, :] * summed
        now = ys[cur, rows, :]
        if k == 0:
            new = (av - CENTER * now) * (1.0 / HALFWIDTH)
        else:
            new = (2.0 / HALFWIDTH) * (av - CENTER * now) - ys[old, rows, :]
        if k < DEGREE - 1:
            ys[old, rows, :] = new
        return new.astype(jnp.bfloat16)

    def place(own_row, n, value):
        rows = pl.ds(own_row, n)
        lb[zh, rows, :] = value
        rb[x, rows, :] = value
        filt_ref[rows, :] = value

    def piece_rows(p):
        off, size = (((1 - c) * ghost, 3 * ghost), (c * 3 * ghost, ghost))[p]
        return pl.ds(pl.multiple_of(off, ghost), size)

    def x_send(i, p):
        slot = x if i < 2 else at("x", toward)
        ref = rb.at[slot, piece_rows(p)]
        return copy(ref, ref, s_r.at[i, p], r_r.at[i, p], beside("x", (1, -1, -toward)[i]))

    def x_recv(i, p):
        ref = rb.at[at("x", (-1, 1, 2)[i]), piece_rows(p)]
        return copy(ref, ref, s_r.at[i, p], r_r.at[i, p], beside("x", (-1, 1, toward)[i]))

    def h_send(i, p):
        slot = zh if i == 0 else at("h", toward)
        ref = lb.at[slot, piece_rows(p)]
        return copy(ref, ref, s_l.at[i, p], r_l.at[i, p], beside("h", -toward))

    def h_recv(i, p):
        ref = lb.at[at("h", toward if i == 0 else 2), piece_rows(p)]
        return copy(ref, ref, s_l.at[i, p], r_l.at[i, p], beside("h", toward))

    def send_piece(p):
        h_send(0, p).start()
        if nx > 1:
            x_send(0, p).start()
            x_send(1, p).start()

    for k in range(DEGREE):
        last = k == DEGREE - 1
        offs = []
        for which in range(2):
            s = side_of(which)
            off = pl.multiple_of(s * own, block)
            offs.append((s, off))
            u = product(pl.ds(off, block))
            us_f[pl.ds(off, block), :] = u
            us[k, s] = u.astype(us.dtype)
            u_send(k, which).start()
        mid = slice(block, own)
        mid_new = advance(k, mid, product(mid))
        if last:
            place(ghost, own - block, mid_new)
        fresh = []
        for which in (1, 0):
            s, off = offs[which]
            u_recv(k, which).wait_recv()
            if not last:
                rows = pl.ds(off, block)
                fresh.append((rows, advance(
                    k, rows, us_f[rows, :] + ur[k, s].astype(jnp.float32))))
            else:
                inner = pl.multiple_of((1 - s) * ghost, ghost)
                rows = pl.ds(pl.multiple_of(off + inner, ghost), ghost)
                new = advance(
                    k, rows,
                    us_f[rows, :] + ur[k, s, pl.ds(inner, ghost), :].astype(jnp.float32))
                place(pl.multiple_of(s * 3 * ghost, ghost), ghost, new)
                send_piece(1 - which)
        if not last:
            vext[mid, :] = mid_new
            for rows, value in fresh:
                vext[rows, :] = value

    for p in range(2):
        if nx > 1:
            for i in range(2):
                x_recv(i, p).wait_recv()
            x_send(2, p).start()
        h_recv(0, p).wait_recv()
        h_send(1, p).start()
    if nx > 1:
        for p in range(2):
            x_recv(2, p).wait_recv()

    def over_nodes(left_op, right_op):
        return lax.dot_general(left_op, right_op, (((0,), (0,)), ((), ())),
                               preferred_element_type=jnp.float32)

    right_op = jnp.concatenate([rb[xx] for xx in range(nx)], axis=1)
    p_copy = copy(pp.at[1], px, s_p.at[0], r_p.at[0], partner)

    def e_copy(src, dst, send, recv, xx):
        return copy(src.at[xx], dst.at[y], send.at[xx], recv.at[y], dev(xx, x, zh, zl, c))

    def e_away(xx):
        return jnp.logical_not((x == xx) & (x == y))

    def spread_out(value_of, src, dst, send, recv):
        for xx in range(nx):
            value = value_of(slice(xx * width, (xx + 1) * width)).astype(src.dtype)

            @pl.when(e_away(xx))
            def _(xx=xx, value=value):
                src[xx] = value
                e_copy(src, dst, send, recv, xx).start()

            @pl.when(jnp.logical_not(e_away(xx)))
            def _(value=value):
                dst[y] = value

    def collected(dst, send, recv):
        acc = None
        for yy in range(ny):
            here = copy(dst.at[yy], dst.at[yy], send.at[yy], recv.at[yy], dev(y, yy, zh, zl, c))
            pl.when(jnp.logical_not((x == y) & (y == yy)))(here.wait_recv)
            term = dst[yy].astype(jnp.float32)
            acc = term if acc is None else acc + term
        return acc

    def em_send(xx):
        return copy(esm.at[xx], erm.at[y], s_em.at[xx], r_em.at[y], dev(x, xx, zh, zl, c))

    def z_target(j):
        kept = at("h", toward) if j >= 4 else jnp.where(c == 0, zh, at("h", 2))
        return kept * 2 + (j // 2) % 2, j % 2

    def z_away(j):
        lz, core = z_target(j)
        return jnp.logical_not((zl == lz) & (c == core))

    def z_send(j):
        lz, core = z_target(j)
        return copy(zs.at[j * out_rows:(j + 1) * out_rows], zr.at[zl], s_z.at[j], r_z.at[zl],
                    dev(x, y, zh, lz, core))

    def z_recv(lz):
        return copy(zr.at[lz], zr.at[lz], s_z.at[lz], r_z.at[lz], dev(x, y, zh, lz, half))

    def hand_over(which, value):
        zs[which * width:(which + 1) * width, :] = value.astype(zs.dtype)
        for j in range(4 * which, 4 * which + 4):
            pl.when(z_away(j))(lambda j=j: z_send(j).start())

            @pl.when(jnp.logical_not(z_away(j)))
            def _(j=j):
                zr[zl] = zs[j * out_rows:(j + 1) * out_rows, :]

    side = lb[at("h", toward)]
    for xx in range(nx):
        value = over_nodes(rb[xx], side).astype(esm.dtype)

        @pl.when(y != xx)
        def _(xx=xx, value=value):
            esm[xx] = value
            em_send(xx).start()

        @pl.when(y == xx)
        def _(value=value):
            erm[y] = value
    pb[...] = over_nodes(side, right_op)
    spread_out(lambda cols: pb[:, cols], esb, erb, s_eb, r_eb)
    pp[c] = over_nodes(lb[zh], right_op)
    pl.when(c == 1)(p_copy.start)

    acc = None
    for yy in range(ny):
        here = copy(erm.at[yy], erm.at[yy], s_em.at[yy], r_em.at[yy], dev(x, yy, zh, zl, c))
        pl.when(y != yy)(here.wait_recv)
        term = erm[yy].astype(jnp.float32)
        acc = term if acc is None else acc + term
    ms[...] = acc.astype(ms.dtype)
    m_copy = copy(ms, mr, s_m.at[0], r_m.at[0], mirror)
    m_copy.start()
    kept = collected(erb, s_eb, r_eb)

    for p in range(2):
        h_recv(1, p).wait_recv()
    pp[1 - c] = over_nodes(lb[at("h", 2)], right_op)
    pl.when(c == 0)(p_copy.start)
    p_copy.wait_recv()
    spread_out(lambda cols: pp[0, :, cols] + px[:, cols], esa, era, s_ea, r_ea)
    m_copy.wait_recv()
    hand_over(1, kept + mr[...].astype(jnp.float32))
    hand_over(0, collected(era, s_ea, r_ea))

    acc = None
    for lz in range(nz):
        pl.when(jnp.logical_not((zl == lz) & (c == half)))(lambda lz=lz: z_recv(lz).wait_recv())
        term = zr[lz].astype(jnp.float32)
        acc = term if acc is None else acc + term
    marg_ref[...] = acc * (1.0 / float(own * domains) ** 0.5)

    for k in range(DEGREE):
        for which in range(2):
            u_send(k, which).wait_send()
    for p in range(2):
        for i in range(2):
            h_send(i, p).wait_send()
        for i in range(3 if nx > 1 else 0):
            x_send(i, p).wait_send()
    p_copy.wait_send()
    m_copy.wait_send()
    for xx in range(nx):
        @pl.when(e_away(xx))
        def _(xx=xx):
            e_copy(esa, era, s_ea, r_ea, xx).wait_send()
            e_copy(esb, erb, s_eb, r_eb, xx).wait_send()
        pl.when(y != xx)(lambda xx=xx: em_send(xx).wait_send())
    for j in range(8):
        pl.when(z_away(j))(lambda j=j: z_send(j).wait_send())


def local(shape, wavefunctions, cell_ham, connectivity, inv_mass, cell_count):
    nx, ny, nh, nz = shape
    own, width = wavefunctions.shape
    cells, npc, _ = cell_ham.shape
    ghost = own // 4
    ext = own + 2 * ghost
    block = 2 * ghost
    out_rows = width // 4
    bf, f32 = jnp.bfloat16, jnp.float32
    sent = bf
    dma = pltpu.SemaphoreType.DMA
    vm = pl.BlockSpec(memory_space=pltpu.VMEM)
    hbm = pl.BlockSpec(memory_space=pl.ANY)
    filtered, rows = pl.pallas_call(
        functools.partial(kernel, shape),
        out_shape=(jax.ShapeDtypeStruct((own, width), bf), jax.ShapeDtypeStruct((out_rows, width), f32)),
        in_specs=[hbm, hbm, hbm, hbm, pl.BlockSpec(memory_space=pltpu.SMEM)],
        out_specs=(vm, vm),
        scratch_shapes=[
            pltpu.VMEM((cells, npc, npc), bf),
            pltpu.VMEM((cells, npc), jnp.int32),
            pltpu.VMEM((4, ghost), f32),
            dma((4,)),
            pltpu.VMEM((ext, cells * npc), bf),
            pltpu.VMEM((cells * npc, ext), bf),
            pltpu.VMEM((cells * npc, ext), bf),
            pltpu.VMEM((ext, ext), bf),
            pltpu.VMEM((ext, ext), bf),
            pltpu.VMEM((ext, width), f32),
            pltpu.VMEM((2, 4, ghost), f32),
            pltpu.VMEM((ext, width), bf),
            pltpu.VMEM((2, ext, width), f32),
            pltpu.VMEM((ext, width), f32),
            pltpu.VMEM((DEGREE, 2, block, width), sent),
            pltpu.VMEM((DEGREE, 2, block, width), sent),
            pltpu.VMEM((nx, own, width), bf),
            pltpu.VMEM((nh, own, width), bf),
            pltpu.VMEM((2, width, nx * width), f32),
            pltpu.VMEM((width, nx * width), f32),
            pltpu.VMEM((width, nx * width), f32),
            pltpu.VMEM((nx, width, width), bf),
            pltpu.VMEM((ny, width, width), bf),
            pltpu.VMEM((nx, width, width), bf),
            pltpu.VMEM((ny, width, width), bf),
            pltpu.VMEM((nx, width, width), bf),
            pltpu.VMEM((ny, width, width), bf),
            pltpu.VMEM((width, width), bf),
            pltpu.VMEM((width, width), bf),
            pltpu.VMEM((2 * width, width), bf),
            pltpu.VMEM((nz, out_rows, width), bf),
            dma((2,)), dma((2,)), dma((2,)), dma((2,)),
            dma((DEGREE, 2)), dma((DEGREE, 2)),
            dma((3, 2)), dma((3, 2)), dma((2, 2)), dma((2, 2)),
            dma((1,)), dma((1,)),
            dma((nx,)), dma((ny,)), dma((nx,)), dma((ny,)), dma((nx,)), dma((ny,)),
            dma((1,)), dma((1,)),
            dma((8,)), dma((nz,)),
        ],
        compiler_params=pltpu.CompilerParams(
            collective_id=0, has_side_effects=True, vmem_limit_bytes=67043328),
        name="filter_margin",
    )(wavefunctions, cell_ham, connectivity, inv_mass.reshape(4, ghost), cell_count)
    return filtered, rows.T


def solution(mesh, shape=(NX, NY, NH, NZ)):
    return jax.shard_map(
        functools.partial(local, shape), mesh=mesh,
        in_specs=(P("dom", "band"), P("dom", None, None), P("dom", None), P("dom"), P("dom")),
        out_specs=(P("dom", "band"), P("band", "dom")),
        check_vma=False,
    )
```

```python
import functools

import jax
import jax.numpy as jnp
from jax import lax
from jax.experimental import pallas as pl
from jax.experimental.pallas import tpu as pltpu
from jax.sharding import PartitionSpec as P

DEGREE = 4
CENTER = 0.5
HALFWIDTH = 3.0
NX, NY, NH, NZ = 4, 4, 4, 8
PACED = 2
MESH = pl.DeviceIdType.MESH


def tile_of(size, most):
    return most if size % most == 0 else size


def kernel(
    shape, w_hbm, h_hbm, conn_hbm, im_hbm, cnt_ref, filt_ref, marg_ref,
    h_ref, conn_ref, im_ref, s_in,
    st, thi, tlo, ahi, alo, mext, imx, vext, ys, us_f, upart, us, ur, rb, lb, pp, px, pb,
    esa, era, esb, erb, esm, erm, ms, mr, zs, zr,
    s_w, r_w, s_im, r_im, s_u, r_u, s_r, r_r, s_l, r_l, s_p, r_p, s_ea, r_ea, s_eb, r_eb, s_em, r_em, s_m, r_m, s_z, r_z,
):
    nx, ny, nh, nz = shape
    own, width = w_hbm.shape
    cells, npc, _ = h_ref.shape
    ghost = own // 4
    ext = own + 2 * ghost
    block = 2 * ghost
    out_rows = width // 4
    domains = ny * nz * 2

    d = lax.axis_index("dom")
    b = lax.axis_index("band")
    c = lax.rem(d, 2)
    zl = lax.rem(lax.div(d, 2), nz)
    y = lax.div(d, 2 * nz)
    zh = lax.rem(b, nh)
    x = lax.div(b, nh)

    def dev(xx, yy, hz, lz, core):
        return ((yy * nz + lz) * 2 + core, xx * nh + hz)

    def copy(src, dst, send, recv, where):
        return pltpu.make_async_remote_copy(
            src_ref=src, dst_ref=dst, send_sem=send, recv_sem=recv,
            device_id=where, device_id_type=MESH,
        )

    ring = {"h": (zh, nh), "x": (x, nx)}

    def at(axis, step):
        place, count = ring[axis]
        return lax.rem(place + count + step, count)

    def beside(axis, step):
        if axis == "h":
            return dev(x, y, at("h", step), zl, c)
        return dev(at("x", step), y, zh, zl, c)

    loads = [
        pltpu.make_async_copy(w_hbm, vext.at[slice(ghost, ghost + own)], s_in.at[0]),
        pltpu.make_async_copy(im_hbm, im_ref, s_in.at[1]),
        pltpu.make_async_copy(conn_hbm, conn_ref, s_in.at[2]),
        pltpu.make_async_copy(h_hbm, h_ref, s_in.at[3]),
    ]
    for one in loads:
        one.start()

    toward = 2 * c - 1
    mirror = dev(x, y, at("h", toward), zl, 1 - c)

    barrier = pltpu.get_barrier_semaphore()

    def greet(where):
        pl.semaphore_signal(barrier, inc=1, device_id=where, device_id_type=MESH)

    left = (lax.rem(d + domains - 1, domains), b)
    right = (lax.rem(d + 1, domains), b)
    greet(left)
    greet(right)
    greet(beside("h", toward))
    greet(mirror)
    if nx > 1:
        greet(beside("x", 1))
        greet(beside("x", -1))
    partner = dev(x, y, zh, zl, 1 - c)
    greet(partner)
    for yy in range(ny):
        pl.when(jnp.logical_not((x == y) & (y == yy)))(
            functools.partial(greet, dev(y, yy, zh, zl, c)))
    for yy in range(ny):
        pl.when(y != yy)(functools.partial(greet, dev(x, yy, zh, zl, c)))
    ahead = lax.rem(lax.div(zl, 2) + nh - zh, nh)
    half = jnp.where((ahead == 1) | (ahead == 2), 1, 0)
    for lz in range(nz):
        pl.when(jnp.logical_not((zl == lz) & (c == half)))(
            functools.partial(greet, dev(x, y, zh, lz, half)))

    for one in loads[2:]:
        one.wait()

    for cell in range(cells):
        live = cell < cnt_ref[0]
        cols = slice(cell * npc, (cell + 1) * npc)
        rt = tile_of(ext, 128)
        for r in range(ext // rt):
            ids = lax.broadcasted_iota(jnp.int32, (rt, npc), 0) + r * rt
            hit = (conn_ref[cell:cell + 1, :] == ids) & live
            st[r * rt:(r + 1) * rt, cols] = jnp.where(hit, 1.0, 0.0).astype(jnp.bfloat16)

    rt = tile_of(npc, 256)
    ct = tile_of(ext, 256)
    for cell in range(cells):
        def gather_cols(i, carry, cell=cell):
            r = pl.multiple_of(lax.div(i, ext // ct) * rt, rt)
            e = pl.multiple_of(lax.rem(i, ext // ct) * ct, ct)
            t = lax.dot_general(
                h_ref[cell, pl.ds(r, rt), :], st[pl.ds(e, ct), cell * npc:(cell + 1) * npc],
                (((1,), (1,)), ((), ())), preferred_element_type=jnp.float32)
            hi = t.astype(jnp.bfloat16)
            thi[pl.ds(cell * npc + r, rt), pl.ds(e, ct)] = hi
            tlo[pl.ds(cell * npc + r, rt), pl.ds(e, ct)] = (t - hi.astype(jnp.float32)).astype(jnp.bfloat16)
            return carry
        lax.fori_loop(0, (npc // rt) * (ext // ct), gather_cols, 0)

    loads[0].wait()
    loads[1].wait()
    as_int = lambda flag: flag.astype(jnp.int32)
    total = (2 + 2 + (2 if nx > 1 else 0) + 1 + (nx - as_int(x == y)) + (ny - 1)
             + (nz - as_int(half == c)))
    pl.semaphore_wait(barrier, total)

    first = []
    for side, where in ((0, left), (1, right)):
        other = 1 - side
        rows = slice(ghost, 2 * ghost) if side == 0 else slice(own, own + ghost)
        land = slice(own + ghost, ext) if side == 0 else slice(0, ghost)
        first.append(copy(im_ref, imx.at[other], s_im.at[side], r_im.at[other], where))
        first.append(copy(vext.at[rows], vext.at[land], s_w.at[side], r_w.at[other], where))
    for one in first:
        one.start()
    art = tile_of(ext, 256)

    def scatter_rows(i, carry):
        r = pl.multiple_of(lax.div(i, ext // ct) * art, art)
        e = pl.multiple_of(lax.rem(i, ext // ct) * ct, ct)
        rows = st[pl.ds(r, art), :]
        a = jnp.dot(rows, thi[:, pl.ds(e, ct)], preferred_element_type=jnp.float32)
        a += jnp.dot(rows, tlo[:, pl.ds(e, ct)], preferred_element_type=jnp.float32)
        hi = a.astype(jnp.bfloat16)
        ahi[pl.ds(r, art), pl.ds(e, ct)] = hi
        alo[pl.ds(r, art), pl.ds(e, ct)] = (a - hi.astype(jnp.float32)).astype(jnp.bfloat16)
        return carry
    lax.fori_loop(0, (ext // art) * (ext // ct), scatter_rows, 0)

    def column(row):
        return jnp.transpose(jnp.broadcast_to(row, (row.shape[1], row.shape[1])))[:, :1]

    def spread(row):
        return jnp.broadcast_to(column(row), (ghost, width))

    for i in range(4):
        mext[ghost * (i + 1):ghost * (i + 2), :] = spread(im_ref[i:i + 1, :])
    for one in first:
        one.wait()
    mext[0:ghost, :] = spread(imx[0, 3:4, :])
    mext[own + ghost:ext, :] = spread(imx[1, 0:1, :])
    ys[0] = vext[...].astype(jnp.float32)

    def side_of(which):
        return c if which == 0 else 1 - c

    def u_send(k, which):
        s = side_of(which)
        where = (lax.rem(d + domains + 2 * s - 1, domains), b)
        if k < DEGREE - 1:
            src, dst = us.at[k, s], ur.at[k, 1 - s]
        else:
            out = pl.ds(pl.multiple_of(s * ghost, ghost), ghost)
            src, dst = us.at[k, s, out], ur.at[k, 1 - s, out]
        return copy(src, dst, s_u.at[k, s], r_u.at[k, 1 - s], where)

    def u_recv(k, which):
        s = side_of(which)
        where = (lax.rem(d + domains + 2 * s - 1, domains), b)
        got = ur.at[k, s]
        if k == DEGREE - 1:
            got = ur.at[k, s, pl.ds(pl.multiple_of((1 - s) * ghost, ghost), ghost)]
        return copy(got, got, s_u.at[k, s], r_u.at[k, s], where)

    def product(rows):
        v = vext[...]
        return (jnp.dot(ahi[rows, :], v, preferred_element_type=jnp.float32)
                + jnp.dot(alo[rows, :], v, preferred_element_type=jnp.float32))

    def advance(k, rows, summed):
        cur, old = k % 2, 1 - k % 2
        av = mext[rows, :] * summed
        now = ys[cur, rows, :]
        if k == 0:
            new = (av - CENTER * now) * (1.0 / HALFWIDTH)
        else:
            new = (2.0 / HALFWIDTH) * (av - CENTER * now) - ys[old, rows, :]
        if k < DEGREE - 1:
            ys[old, rows, :] = new
        return new.astype(jnp.bfloat16)

    def place(own_row, n, value):
        rows = pl.ds(own_row, n)
        lb[zh, rows, :] = value
        rb[x, rows, :] = value
        filt_ref[rows, :] = value

    def piece_rows(p):
        off, size = (((1 - c) * ghost, 3 * ghost), (c * 3 * ghost, ghost))[p]
        return pl.ds(pl.multiple_of(off, ghost), size)

    def x_send(i, p):
        slot = x if i < 2 else at("x", toward)
        ref = rb.at[slot, piece_rows(p)]
        return copy(ref, ref, s_r.at[i, p], r_r.at[i, p], beside("x", (1, -1, -toward)[i]))

    def x_recv(i, p):
        ref = rb.at[at("x", (-1, 1, 2)[i]), piece_rows(p)]
        return copy(ref, ref, s_r.at[i, p], r_r.at[i, p], beside("x", (-1, 1, toward)[i]))

    def chunk_rows(q):
        off = (q + 1 - c) * ghost if q < 3 else c * 3 * ghost
        return pl.ds(pl.multiple_of(off, ghost), ghost)

    def h_send(i, q):
        slot = zh if i == 0 else at("h", toward)
        ref = lb.at[slot, chunk_rows(q)]
        return copy(ref, ref, s_l.at[i, q], r_l.at[i, q], beside("h", -toward))

    def h_recv(i, q):
        ref = lb.at[at("h", toward if i == 0 else 2), chunk_rows(q)]
        return copy(ref, ref, s_l.at[i, q], r_l.at[i, q], beside("h", toward))

    paced = (zl >= PACED) & (zl < nz - PACED)

    def send_piece(p):
        if p == 0:
            h_send(0, 0).start()
            h_send(0, 1).start()
            pl.when(jnp.logical_not(paced))(lambda: h_send(0, 2).start())
        else:
            pl.when(jnp.logical_not(paced))(lambda: h_send(0, 3).start())
        if nx > 1:
            x_send(0, p).start()
            x_send(1, p).start()

    far_rows = pl.ds(pl.multiple_of(c * own, block), block)
    near_rows = pl.ds(pl.multiple_of((1 - c) * own, block), block)
    rest_rows = pl.ds(pl.multiple_of((1 - c) * block, block), own)
    mid = slice(block, own)

    def part_product(rows, cols):
        v = vext[cols, :]
        return (jnp.dot(ahi[rows, cols], v, preferred_element_type=jnp.float32)
                + jnp.dot(alo[rows, cols], v, preferred_element_type=jnp.float32))

    def emit(k, which, rows, u):
        us_f[rows, :] = u
        us[k, side_of(which)] = u.astype(us.dtype)
        u_send(k, which).start()

    def settle(k, which, rows):
        s = side_of(which)
        u_recv(k, which).wait_recv()
        if k < DEGREE - 1:
            return advance(k, rows, us_f[rows, :] + ur[k, s].astype(jnp.float32))
        inner = pl.multiple_of((1 - s) * ghost, ghost)
        rows = pl.ds(pl.multiple_of(s * own + inner, ghost), ghost)
        new = advance(
            k, rows, us_f[rows, :] + ur[k, s, pl.ds(inner, ghost), :].astype(jnp.float32))
        place(pl.multiple_of(s * 3 * ghost, ghost), ghost, new)
        send_piece(1 - which)
        return None

    for k in range(DEGREE):
        last = k == DEGREE - 1
        if k == 0:
            emit(k, 0, far_rows, product(far_rows))
        else:
            emit(k, 0, far_rows, upart[...] + part_product(far_rows, far_rows))
        emit(k, 1, near_rows, product(near_rows))
        mid_new = advance(k, mid, product(mid))
        if last:
            place(ghost, own - block, mid_new)
            settle(k, 1, near_rows)
            settle(k, 0, far_rows)
        else:
            near_new = settle(k, 1, near_rows)
            vext[mid, :] = mid_new
            vext[near_rows, :] = near_new
            upart[...] = part_product(far_rows, rest_rows)
            vext[far_rows, :] = settle(k, 0, far_rows)

    for p in range(2):
        if nx > 1:
            for i in range(2):
                x_recv(i, p).wait_recv()
            x_send(2, p).start()
        for q in ((0, 1, 2), (3,))[p]:
            h_recv(0, q).wait_recv()
            if q == 1:
                @pl.when(paced)
                def _():
                    h_send(0, 2).start()
                    h_send(0, 3).start()
            h_send(1, q).start()
    if nx > 1:
        for p in range(2):
            x_recv(2, p).wait_recv()

    def over_nodes(left_op, right_op):
        return lax.dot_general(left_op, right_op, (((0,), (0,)), ((), ())),
                               preferred_element_type=jnp.float32)

    right_op = jnp.concatenate([rb[xx] for xx in range(nx)], axis=1)
    p_copy = copy(pp.at[1], px, s_p.at[0], r_p.at[0], partner)

    def e_copy(src, dst, send, recv, xx):
        return copy(src.at[xx], dst.at[y], send.at[xx], recv.at[y], dev(xx, x, zh, zl, c))

    def e_away(xx):
        return jnp.logical_not((x == xx) & (x == y))

    def spread_out(value_of, src, dst, send, recv):
        for xx in range(nx):
            value = value_of(slice(xx * width, (xx + 1) * width)).astype(src.dtype)

            @pl.when(e_away(xx))
            def _(xx=xx, value=value):
                src[xx] = value
                e_copy(src, dst, send, recv, xx).start()

            @pl.when(jnp.logical_not(e_away(xx)))
            def _(value=value):
                dst[y] = value

    def collected(dst, send, recv):
        acc = None
        for yy in range(ny):
            here = copy(dst.at[yy], dst.at[yy], send.at[yy], recv.at[yy], dev(y, yy, zh, zl, c))
            pl.when(jnp.logical_not((x == y) & (y == yy)))(here.wait_recv)
            term = dst[yy].astype(jnp.float32)
            acc = term if acc is None else acc + term
        return acc

    def em_send(xx):
        return copy(esm.at[xx], erm.at[y], s_em.at[xx], r_em.at[y], dev(x, xx, zh, zl, c))

    def z_target(j):
        kept = at("h", toward) if j >= 4 else jnp.where(c == 0, zh, at("h", 2))
        return kept * 2 + (j // 2) % 2, j % 2

    def z_away(j):
        lz, core = z_target(j)
        return jnp.logical_not((zl == lz) & (c == core))

    def z_send(j):
        lz, core = z_target(j)
        return copy(zs.at[j * out_rows:(j + 1) * out_rows], zr.at[zl], s_z.at[j], r_z.at[zl],
                    dev(x, y, zh, lz, core))

    def z_recv(lz):
        return copy(zr.at[lz], zr.at[lz], s_z.at[lz], r_z.at[lz], dev(x, y, zh, lz, half))

    def hand_over(which, value):
        zs[which * width:(which + 1) * width, :] = value.astype(zs.dtype)
        for j in range(4 * which, 4 * which + 4):
            pl.when(z_away(j))(lambda j=j: z_send(j).start())

            @pl.when(jnp.logical_not(z_away(j)))
            def _(j=j):
                zr[zl] = zs[j * out_rows:(j + 1) * out_rows, :]

    side = lb[at("h", toward)]
    for xx in range(nx):
        value = over_nodes(rb[xx], side).astype(esm.dtype)

        @pl.when(y != xx)
        def _(xx=xx, value=value):
            esm[xx] = value
            em_send(xx).start()

        @pl.when(y == xx)
        def _(value=value):
            erm[y] = value
    pb[...] = over_nodes(side, right_op)
    spread_out(lambda cols: pb[:, cols], esb, erb, s_eb, r_eb)
    pp[c] = over_nodes(lb[zh], right_op)
    pl.when(c == 1)(p_copy.start)

    acc = None
    for yy in range(ny):
        here = copy(erm.at[yy], erm.at[yy], s_em.at[yy], r_em.at[yy], dev(x, yy, zh, zl, c))
        pl.when(y != yy)(here.wait_recv)
        term = erm[yy].astype(jnp.float32)
        acc = term if acc is None else acc + term
    ms[...] = acc.astype(ms.dtype)
    m_copy = copy(ms, mr, s_m.at[0], r_m.at[0], mirror)
    m_copy.start()
    kept = collected(erb, s_eb, r_eb)

    for q in range(4):
        h_recv(1, q).wait_recv()
    pp[1 - c] = over_nodes(lb[at("h", 2)], right_op)
    pl.when(c == 0)(p_copy.start)
    p_copy.wait_recv()
    spread_out(lambda cols: pp[0, :, cols] + px[:, cols], esa, era, s_ea, r_ea)
    m_copy.wait_recv()
    hand_over(1, kept + mr[...].astype(jnp.float32))
    hand_over(0, collected(era, s_ea, r_ea))

    acc = None
    for lz in range(nz):
        pl.when(jnp.logical_not((zl == lz) & (c == half)))(lambda lz=lz: z_recv(lz).wait_recv())
        term = zr[lz].astype(jnp.float32)
        acc = term if acc is None else acc + term
    marg_ref[...] = acc * (1.0 / float(own * domains) ** 0.5)

    for k in range(DEGREE):
        for which in range(2):
            u_send(k, which).wait_send()
    for p in range(2):
        for q in range(4 if p == 0 else 0):
            h_send(0, q).wait_send()
            h_send(1, q).wait_send()
        for i in range(3 if nx > 1 else 0):
            x_send(i, p).wait_send()
    p_copy.wait_send()
    m_copy.wait_send()
    for xx in range(nx):
        @pl.when(e_away(xx))
        def _(xx=xx):
            e_copy(esa, era, s_ea, r_ea, xx).wait_send()
            e_copy(esb, erb, s_eb, r_eb, xx).wait_send()
        pl.when(y != xx)(lambda xx=xx: em_send(xx).wait_send())
    for j in range(8):
        pl.when(z_away(j))(lambda j=j: z_send(j).wait_send())


def local(shape, wavefunctions, cell_ham, connectivity, inv_mass, cell_count):
    nx, ny, nh, nz = shape
    own, width = wavefunctions.shape
    cells, npc, _ = cell_ham.shape
    ghost = own // 4
    ext = own + 2 * ghost
    block = 2 * ghost
    out_rows = width // 4
    bf, f32 = jnp.bfloat16, jnp.float32
    sent = bf
    dma = pltpu.SemaphoreType.DMA
    vm = pl.BlockSpec(memory_space=pltpu.VMEM)
    hbm = pl.BlockSpec(memory_space=pl.ANY)
    filtered, rows = pl.pallas_call(
        functools.partial(kernel, shape),
        out_shape=(jax.ShapeDtypeStruct((own, width), bf), jax.ShapeDtypeStruct((out_rows, width), f32)),
        in_specs=[hbm, hbm, hbm, hbm, pl.BlockSpec(memory_space=pltpu.SMEM)],
        out_specs=(vm, vm),
        scratch_shapes=[
            pltpu.VMEM((cells, npc, npc), bf),
            pltpu.VMEM((cells, npc), jnp.int32),
            pltpu.VMEM((4, ghost), f32),
            dma((4,)),
            pltpu.VMEM((ext, cells * npc), bf),
            pltpu.VMEM((cells * npc, ext), bf),
            pltpu.VMEM((cells * npc, ext), bf),
            pltpu.VMEM((ext, ext), bf),
            pltpu.VMEM((ext, ext), bf),
            pltpu.VMEM((ext, width), f32),
            pltpu.VMEM((2, 4, ghost), f32),
            pltpu.VMEM((ext, width), bf),
            pltpu.VMEM((2, ext, width), f32),
            pltpu.VMEM((ext, width), f32),
            pltpu.VMEM((block, width), f32),
            pltpu.VMEM((DEGREE, 2, block, width), sent),
            pltpu.VMEM((DEGREE, 2, block, width), sent),
            pltpu.VMEM((nx, own, width), bf),
            pltpu.VMEM((nh, own, width), bf),
            pltpu.VMEM((2, width, nx * width), f32),
            pltpu.VMEM((width, nx * width), f32),
            pltpu.VMEM((width, nx * width), f32),
            pltpu.VMEM((nx, width, width), bf),
            pltpu.VMEM((ny, width, width), bf),
            pltpu.VMEM((nx, width, width), bf),
            pltpu.VMEM((ny, width, width), bf),
            pltpu.VMEM((nx, width, width), bf),
            pltpu.VMEM((ny, width, width), bf),
            pltpu.VMEM((width, width), bf),
            pltpu.VMEM((width, width), bf),
            pltpu.VMEM((2 * width, width), bf),
            pltpu.VMEM((nz, out_rows, width), bf),
            dma((2,)), dma((2,)), dma((2,)), dma((2,)),
            dma((DEGREE, 2)), dma((DEGREE, 2)),
            dma((3, 2)), dma((3, 2)), dma((2, 4)), dma((2, 4)),
            dma((1,)), dma((1,)),
            dma((nx,)), dma((ny,)), dma((nx,)), dma((ny,)), dma((nx,)), dma((ny,)),
            dma((1,)), dma((1,)),
            dma((8,)), dma((nz,)),
        ],
        compiler_params=pltpu.CompilerParams(
            collective_id=0, has_side_effects=True, vmem_limit_bytes=67043328),
        name="filter_margin",
    )(wavefunctions, cell_ham, connectivity, inv_mass.reshape(4, ghost), cell_count)
    return filtered, rows.T


def solution(mesh, shape=(NX, NY, NH, NZ)):
    return jax.shard_map(
        functools.partial(local, shape), mesh=mesh,
        in_specs=(P("dom", "band"), P("dom", None, None), P("dom", None), P("dom"), P("dom")),
        out_specs=(P("dom", "band"), P("band", "dom")),
        check_vma=False,
    )
```

```python
import functools

import jax
import jax.numpy as jnp
from jax import lax
from jax.experimental import pallas as pl
from jax.experimental.pallas import tpu as pltpu
from jax.sharding import PartitionSpec as P

DEGREE = 4
CENTER = 0.5
HALFWIDTH = 3.0
NX, NY, NH, NZ = 4, 4, 4, 8
PACED = 2
MESH = pl.DeviceIdType.MESH


def tile_of(size, most):
    return most if size % most == 0 else size


def kernel(
    shape, w_hbm, h_hbm, conn_hbm, im_hbm, cnt_ref, filt_ref, marg_ref,
    h_ref, conn_ref, im_ref, s_in,
    st, thi, tlo, ahi, alo, mext, imx, vext, ys, us_f, upart, us, ur, rb, lb, pp, px, pb,
    esa, era, esb, erb, esm, erm, ms, mr, zs, zr,
    s_w, r_w, s_im, r_im, s_u, r_u, s_r, r_r, s_l, r_l, s_p, r_p, s_ea, r_ea, s_eb, r_eb, s_em, r_em, s_m, r_m, s_z, r_z,
):
    nx, ny, nh, nz = shape
    own, width = w_hbm.shape
    cells, npc, _ = h_ref.shape
    ghost = own // 4
    ext = own + 2 * ghost
    block = 2 * ghost
    out_rows = width // 4
    domains = ny * nz * 2

    d = lax.axis_index("dom")
    b = lax.axis_index("band")
    c = lax.rem(d, 2)
    zl = lax.rem(lax.div(d, 2), nz)
    y = lax.div(d, 2 * nz)
    zh = lax.rem(b, nh)
    x = lax.div(b, nh)

    def dev(xx, yy, hz, lz, core):
        return ((yy * nz + lz) * 2 + core, xx * nh + hz)

    def copy(src, dst, send, recv, where):
        return pltpu.make_async_remote_copy(
            src_ref=src, dst_ref=dst, send_sem=send, recv_sem=recv,
            device_id=where, device_id_type=MESH,
        )

    ring = {"h": (zh, nh), "x": (x, nx)}

    def at(axis, step):
        place, count = ring[axis]
        return lax.rem(place + count + step, count)

    def beside(axis, step):
        if axis == "h":
            return dev(x, y, at("h", step), zl, c)
        return dev(at("x", step), y, zh, zl, c)

    loads = [
        pltpu.make_async_copy(w_hbm, vext.at[slice(ghost, ghost + own)], s_in.at[0]),
        pltpu.make_async_copy(im_hbm, im_ref, s_in.at[1]),
        pltpu.make_async_copy(conn_hbm, conn_ref, s_in.at[2]),
        pltpu.make_async_copy(h_hbm, h_ref, s_in.at[3]),
    ]
    for one in loads:
        one.start()

    toward = 2 * c - 1
    mirror = dev(x, y, at("h", toward), zl, 1 - c)

    barrier = pltpu.get_barrier_semaphore()

    def greet(where):
        pl.semaphore_signal(barrier, inc=1, device_id=where, device_id_type=MESH)

    left = (lax.rem(d + domains - 1, domains), b)
    right = (lax.rem(d + 1, domains), b)
    greet(left)
    greet(right)
    greet(beside("h", toward))
    greet(mirror)
    if nx > 1:
        greet(beside("x", 1))
        greet(beside("x", -1))
    partner = dev(x, y, zh, zl, 1 - c)
    greet(partner)
    for yy in range(ny):
        pl.when(jnp.logical_not((x == y) & (y == yy)))(
            functools.partial(greet, dev(y, yy, zh, zl, c)))
    for yy in range(ny):
        pl.when(y != yy)(functools.partial(greet, dev(x, yy, zh, zl, c)))
    ahead = lax.rem(lax.div(zl, 2) + nh - zh, nh)
    half = jnp.where((ahead == 1) | (ahead == 2), 1, 0)
    for lz in range(nz):
        pl.when(jnp.logical_not((zl == lz) & (c == half)))(
            functools.partial(greet, dev(x, y, zh, lz, half)))

    for one in loads[2:]:
        one.wait()

    for cell in range(cells):
        live = cell < cnt_ref[0]
        cols = slice(cell * npc, (cell + 1) * npc)
        rt = tile_of(ext, 128)
        for r in range(ext // rt):
            ids = lax.broadcasted_iota(jnp.int32, (rt, npc), 0) + r * rt
            hit = (conn_ref[cell:cell + 1, :] == ids) & live
            st[r * rt:(r + 1) * rt, cols] = jnp.where(hit, 1.0, 0.0).astype(jnp.bfloat16)

    rt = tile_of(npc, 256)
    ct = tile_of(ext, 256)
    for cell in range(cells):
        def gather_cols(i, carry, cell=cell):
            r = pl.multiple_of(lax.div(i, ext // ct) * rt, rt)
            e = pl.multiple_of(lax.rem(i, ext // ct) * ct, ct)
            t = lax.dot_general(
                h_ref[cell, pl.ds(r, rt), :], st[pl.ds(e, ct), cell * npc:(cell + 1) * npc],
                (((1,), (1,)), ((), ())), preferred_element_type=jnp.float32)
            hi = t.astype(jnp.bfloat16)
            thi[pl.ds(cell * npc + r, rt), pl.ds(e, ct)] = hi
            tlo[pl.ds(cell * npc + r, rt), pl.ds(e, ct)] = (t - hi.astype(jnp.float32)).astype(jnp.bfloat16)
            return carry
        lax.fori_loop(0, (npc // rt) * (ext // ct), gather_cols, 0)
        if cell > 0:
            continue
        loads[0].wait()
        loads[1].wait()
        as_int = lambda flag: flag.astype(jnp.int32)
        total = (2 + 2 + (2 if nx > 1 else 0) + 1 + (nx - as_int(x == y)) + (ny - 1)
                 + (nz - as_int(half == c)))
        pl.semaphore_wait(barrier, total)

        first = []
        for side, where in ((0, left), (1, right)):
            other = 1 - side
            rows = slice(ghost, 2 * ghost) if side == 0 else slice(own, own + ghost)
            land = slice(own + ghost, ext) if side == 0 else slice(0, ghost)
            first.append(copy(im_ref, imx.at[other], s_im.at[side], r_im.at[other], where))
            first.append(copy(vext.at[rows], vext.at[land], s_w.at[side], r_w.at[other], where))
        for one in first:
            one.start()

    art = tile_of(ext, 256)

    def scatter_rows(i, carry):
        r = pl.multiple_of(lax.div(i, ext // ct) * art, art)
        e = pl.multiple_of(lax.rem(i, ext // ct) * ct, ct)
        rows = st[pl.ds(r, art), :]
        a = jnp.dot(rows, thi[:, pl.ds(e, ct)], preferred_element_type=jnp.float32)
        a += jnp.dot(rows, tlo[:, pl.ds(e, ct)], preferred_element_type=jnp.float32)
        hi = a.astype(jnp.bfloat16)
        ahi[pl.ds(r, art), pl.ds(e, ct)] = hi
        alo[pl.ds(r, art), pl.ds(e, ct)] = (a - hi.astype(jnp.float32)).astype(jnp.bfloat16)
        return carry
    lax.fori_loop(0, (ext // art) * (ext // ct), scatter_rows, 0)

    def column(row):
        return jnp.transpose(jnp.broadcast_to(row, (row.shape[1], row.shape[1])))[:, :1]

    def spread(row):
        return jnp.broadcast_to(column(row), (ghost, width))

    for i in range(4):
        mext[ghost * (i + 1):ghost * (i + 2), :] = spread(im_ref[i:i + 1, :])
    for one in first:
        one.wait()
    mext[0:ghost, :] = spread(imx[0, 3:4, :])
    mext[own + ghost:ext, :] = spread(imx[1, 0:1, :])
    ys[0] = vext[...].astype(jnp.float32)

    def side_of(which):
        return c if which == 0 else 1 - c

    def u_send(k, which):
        s = side_of(which)
        where = (lax.rem(d + domains + 2 * s - 1, domains), b)
        if k < DEGREE - 1:
            src, dst = us.at[k, s], ur.at[k, 1 - s]
        else:
            out = pl.ds(pl.multiple_of(s * ghost, ghost), ghost)
            src, dst = us.at[k, s, out], ur.at[k, 1 - s, out]
        return copy(src, dst, s_u.at[k, s], r_u.at[k, 1 - s], where)

    def u_recv(k, which):
        s = side_of(which)
        where = (lax.rem(d + domains + 2 * s - 1, domains), b)
        got = ur.at[k, s]
        if k == DEGREE - 1:
            got = ur.at[k, s, pl.ds(pl.multiple_of((1 - s) * ghost, ghost), ghost)]
        return copy(got, got, s_u.at[k, s], r_u.at[k, s], where)

    def product(rows):
        v = vext[...]
        return (jnp.dot(ahi[rows, :], v, preferred_element_type=jnp.float32)
                + jnp.dot(alo[rows, :], v, preferred_element_type=jnp.float32))

    def advance(k, rows, summed):
        cur, old = k % 2, 1 - k % 2
        av = mext[rows, :] * summed
        now = ys[cur, rows, :]
        if k == 0:
            new = (av - CENTER * now) * (1.0 / HALFWIDTH)
        else:
            new = (2.0 / HALFWIDTH) * (av - CENTER * now) - ys[old, rows, :]
        if k < DEGREE - 1:
            ys[old, rows, :] = new
        return new.astype(jnp.bfloat16)

    def place(own_row, n, value):
        rows = pl.ds(own_row, n)
        lb[zh, rows, :] = value
        rb[x, rows, :] = value
        filt_ref[rows, :] = value

    def piece_rows(p):
        off, size = (((1 - c) * ghost, 3 * ghost), (c * 3 * ghost, ghost))[p]
        return pl.ds(pl.multiple_of(off, ghost), size)

    def x_send(i, p):
        slot = x if i < 2 else at("x", toward)
        ref = rb.at[slot, piece_rows(p)]
        return copy(ref, ref, s_r.at[i, p], r_r.at[i, p], beside("x", (1, -1, -toward)[i]))

    def x_recv(i, p):
        ref = rb.at[at("x", (-1, 1, 2)[i]), piece_rows(p)]
        return copy(ref, ref, s_r.at[i, p], r_r.at[i, p], beside("x", (-1, 1, toward)[i]))

    def chunk_rows(q):
        off = (q + 1 - c) * ghost if q < 3 else c * 3 * ghost
        return pl.ds(pl.multiple_of(off, ghost), ghost)

    def h_send(i, q):
        slot = zh if i == 0 else at("h", toward)
        ref = lb.at[slot, chunk_rows(q)]
        return copy(ref, ref, s_l.at[i, q], r_l.at[i, q], beside("h", -toward))

    def h_recv(i, q):
        ref = lb.at[at("h", toward if i == 0 else 2), chunk_rows(q)]
        return copy(ref, ref, s_l.at[i, q], r_l.at[i, q], beside("h", toward))

    paced = (zl >= PACED) & (zl < nz - PACED)

    def send_piece(p):
        if p == 0:
            h_send(0, 0).start()
            h_send(0, 1).start()
            pl.when(jnp.logical_not(paced))(lambda: h_send(0, 2).start())
        else:
            pl.when(jnp.logical_not(paced))(lambda: h_send(0, 3).start())
        if nx > 1:
            x_send(0, p).start()
            x_send(1, p).start()

    far_rows = pl.ds(pl.multiple_of(c * own, block), block)
    near_rows = pl.ds(pl.multiple_of((1 - c) * own, block), block)
    rest_rows = pl.ds(pl.multiple_of((1 - c) * block, block), own)
    mid = slice(block, own)

    def part_product(rows, cols):
        v = vext[cols, :]
        return (jnp.dot(ahi[rows, cols], v, preferred_element_type=jnp.float32)
                + jnp.dot(alo[rows, cols], v, preferred_element_type=jnp.float32))

    def emit(k, which, rows, u):
        us_f[rows, :] = u
        us[k, side_of(which)] = u.astype(us.dtype)
        u_send(k, which).start()

    def settle(k, which, rows):
        s = side_of(which)
        u_recv(k, which).wait_recv()
        if k < DEGREE - 1:
            return advance(k, rows, us_f[rows, :] + ur[k, s].astype(jnp.float32))
        inner = pl.multiple_of((1 - s) * ghost, ghost)
        rows = pl.ds(pl.multiple_of(s * own + inner, ghost), ghost)
        new = advance(
            k, rows, us_f[rows, :] + ur[k, s, pl.ds(inner, ghost), :].astype(jnp.float32))
        place(pl.multiple_of(s * 3 * ghost, ghost), ghost, new)
        send_piece(1 - which)
        return None

    for k in range(DEGREE):
        last = k == DEGREE - 1
        if k == 0:
            emit(k, 0, far_rows, product(far_rows))
        else:
            emit(k, 0, far_rows, upart[...] + part_product(far_rows, far_rows))
        emit(k, 1, near_rows, product(near_rows))
        mid_new = advance(k, mid, product(mid))
        if last:
            place(ghost, own - block, mid_new)
            settle(k, 1, near_rows)
            settle(k, 0, far_rows)
        else:
            near_new = settle(k, 1, near_rows)
            vext[mid, :] = mid_new
            vext[near_rows, :] = near_new
            upart[...] = part_product(far_rows, rest_rows)
            vext[far_rows, :] = settle(k, 0, far_rows)

    for p in range(2):
        if nx > 1:
            for i in range(2):
                x_recv(i, p).wait_recv()
            x_send(2, p).start()
        for q in ((0, 1, 2), (3,))[p]:
            h_recv(0, q).wait_recv()
            if q == 1:
                @pl.when(paced)
                def _():
                    h_send(0, 2).start()
                    h_send(0, 3).start()
            h_send(1, q).start()
    if nx > 1:
        for p in range(2):
            x_recv(2, p).wait_recv()

    def over_nodes(left_op, right_op):
        return lax.dot_general(left_op, right_op, (((0,), (0,)), ((), ())),
                               preferred_element_type=jnp.float32)

    right_op = jnp.concatenate([rb[xx] for xx in range(nx)], axis=1)
    p_copy = copy(pp.at[1], px, s_p.at[0], r_p.at[0], partner)

    def e_copy(src, dst, send, recv, xx):
        return copy(src.at[xx], dst.at[y], send.at[xx], recv.at[y], dev(xx, x, zh, zl, c))

    def e_away(xx):
        return jnp.logical_not((x == xx) & (x == y))

    def spread_out(value_of, src, dst, send, recv):
        for xx in range(nx):
            value = value_of(slice(xx * width, (xx + 1) * width)).astype(src.dtype)

            @pl.when(e_away(xx))
            def _(xx=xx, value=value):
                src[xx] = value
                e_copy(src, dst, send, recv, xx).start()

            @pl.when(jnp.logical_not(e_away(xx)))
            def _(value=value):
                dst[y] = value

    def collected(dst, send, recv):
        acc = None
        for yy in range(ny):
            here = copy(dst.at[yy], dst.at[yy], send.at[yy], recv.at[yy], dev(y, yy, zh, zl, c))
            pl.when(jnp.logical_not((x == y) & (y == yy)))(here.wait_recv)
            term = dst[yy].astype(jnp.float32)
            acc = term if acc is None else acc + term
        return acc

    def em_send(xx):
        return copy(esm.at[xx], erm.at[y], s_em.at[xx], r_em.at[y], dev(x, xx, zh, zl, c))

    def z_target(j):
        kept = at("h", toward) if j >= 4 else jnp.where(c == 0, zh, at("h", 2))
        return kept * 2 + (j // 2) % 2, j % 2

    def z_away(j):
        lz, core = z_target(j)
        return jnp.logical_not((zl == lz) & (c == core))

    def z_send(j):
        lz, core = z_target(j)
        return copy(zs.at[j * out_rows:(j + 1) * out_rows], zr.at[zl], s_z.at[j], r_z.at[zl],
                    dev(x, y, zh, lz, core))

    def z_recv(lz):
        return copy(zr.at[lz], zr.at[lz], s_z.at[lz], r_z.at[lz], dev(x, y, zh, lz, half))

    def hand_over(which, value):
        zs[which * width:(which + 1) * width, :] = value.astype(zs.dtype)
        for j in range(4 * which, 4 * which + 4):
            pl.when(z_away(j))(lambda j=j: z_send(j).start())

            @pl.when(jnp.logical_not(z_away(j)))
            def _(j=j):
                zr[zl] = zs[j * out_rows:(j + 1) * out_rows, :]

    side = lb[at("h", toward)]
    for xx in range(nx):
        value = over_nodes(rb[xx], side).astype(esm.dtype)

        @pl.when(y != xx)
        def _(xx=xx, value=value):
            esm[xx] = value
            em_send(xx).start()

        @pl.when(y == xx)
        def _(value=value):
            erm[y] = value
    pb[...] = over_nodes(side, right_op)
    spread_out(lambda cols: pb[:, cols], esb, erb, s_eb, r_eb)
    pp[c] = over_nodes(lb[zh], right_op)
    pl.when(c == 1)(p_copy.start)

    acc = None
    for yy in range(ny):
        here = copy(erm.at[yy], erm.at[yy], s_em.at[yy], r_em.at[yy], dev(x, yy, zh, zl, c))
        pl.when(y != yy)(here.wait_recv)
        term = erm[yy].astype(jnp.float32)
        acc = term if acc is None else acc + term
    ms[...] = acc.astype(ms.dtype)
    m_copy = copy(ms, mr, s_m.at[0], r_m.at[0], mirror)
    m_copy.start()
    kept = collected(erb, s_eb, r_eb)

    for q in range(4):
        h_recv(1, q).wait_recv()
    pp[1 - c] = over_nodes(lb[at("h", 2)], right_op)
    pl.when(c == 0)(p_copy.start)
    p_copy.wait_recv()
    spread_out(lambda cols: pp[0, :, cols] + px[:, cols], esa, era, s_ea, r_ea)
    m_copy.wait_recv()
    hand_over(1, kept + mr[...].astype(jnp.float32))
    hand_over(0, collected(era, s_ea, r_ea))

    acc = None
    for lz in range(nz):
        pl.when(jnp.logical_not((zl == lz) & (c == half)))(lambda lz=lz: z_recv(lz).wait_recv())
        term = zr[lz].astype(jnp.float32)
        acc = term if acc is None else acc + term
    marg_ref[...] = acc * (1.0 / float(own * domains) ** 0.5)

    for k in range(DEGREE):
        for which in range(2):
            u_send(k, which).wait_send()
    for p in range(2):
        for q in range(4 if p == 0 else 0):
            h_send(0, q).wait_send()
            h_send(1, q).wait_send()
        for i in range(3 if nx > 1 else 0):
            x_send(i, p).wait_send()
    p_copy.wait_send()
    m_copy.wait_send()
    for xx in range(nx):
        @pl.when(e_away(xx))
        def _(xx=xx):
            e_copy(esa, era, s_ea, r_ea, xx).wait_send()
            e_copy(esb, erb, s_eb, r_eb, xx).wait_send()
        pl.when(y != xx)(lambda xx=xx: em_send(xx).wait_send())
    for j in range(8):
        pl.when(z_away(j))(lambda j=j: z_send(j).wait_send())


def local(shape, wavefunctions, cell_ham, connectivity, inv_mass, cell_count):
    nx, ny, nh, nz = shape
    own, width = wavefunctions.shape
    cells, npc, _ = cell_ham.shape
    ghost = own // 4
    ext = own + 2 * ghost
    block = 2 * ghost
    out_rows = width // 4
    bf, f32 = jnp.bfloat16, jnp.float32
    sent = bf
    dma = pltpu.SemaphoreType.DMA
    vm = pl.BlockSpec(memory_space=pltpu.VMEM)
    hbm = pl.BlockSpec(memory_space=pl.ANY)
    filtered, rows = pl.pallas_call(
        functools.partial(kernel, shape),
        out_shape=(jax.ShapeDtypeStruct((own, width), bf), jax.ShapeDtypeStruct((out_rows, width), f32)),
        in_specs=[hbm, hbm, hbm, hbm, pl.BlockSpec(memory_space=pltpu.SMEM)],
        out_specs=(vm, vm),
        scratch_shapes=[
            pltpu.VMEM((cells, npc, npc), bf),
            pltpu.VMEM((cells, npc), jnp.int32),
            pltpu.VMEM((4, ghost), f32),
            dma((4,)),
            pltpu.VMEM((ext, cells * npc), bf),
            pltpu.VMEM((cells * npc, ext), bf),
            pltpu.VMEM((cells * npc, ext), bf),
            pltpu.VMEM((ext, ext), bf),
            pltpu.VMEM((ext, ext), bf),
            pltpu.VMEM((ext, width), f32),
            pltpu.VMEM((2, 4, ghost), f32),
            pltpu.VMEM((ext, width), bf),
            pltpu.VMEM((2, ext, width), f32),
            pltpu.VMEM((ext, width), f32),
            pltpu.VMEM((block, width), f32),
            pltpu.VMEM((DEGREE, 2, block, width), sent),
            pltpu.VMEM((DEGREE, 2, block, width), sent),
            pltpu.VMEM((nx, own, width), bf),
            pltpu.VMEM((nh, own, width), bf),
            pltpu.VMEM((2, width, nx * width), f32),
            pltpu.VMEM((width, nx * width), f32),
            pltpu.VMEM((width, nx * width), f32),
            pltpu.VMEM((nx, width, width), bf),
            pltpu.VMEM((ny, width, width), bf),
            pltpu.VMEM((nx, width, width), bf),
            pltpu.VMEM((ny, width, width), bf),
            pltpu.VMEM((nx, width, width), bf),
            pltpu.VMEM((ny, width, width), bf),
            pltpu.VMEM((width, width), bf),
            pltpu.VMEM((width, width), bf),
            pltpu.VMEM((2 * width, width), bf),
            pltpu.VMEM((nz, out_rows, width), bf),
            dma((2,)), dma((2,)), dma((2,)), dma((2,)),
            dma((DEGREE, 2)), dma((DEGREE, 2)),
            dma((3, 2)), dma((3, 2)), dma((2, 4)), dma((2, 4)),
            dma((1,)), dma((1,)),
            dma((nx,)), dma((ny,)), dma((nx,)), dma((ny,)), dma((nx,)), dma((ny,)),
            dma((1,)), dma((1,)),
            dma((8,)), dma((nz,)),
        ],
        compiler_params=pltpu.CompilerParams(
            collective_id=0, has_side_effects=True, vmem_limit_bytes=67043328),
        name="filter_margin",
    )(wavefunctions, cell_ham, connectivity, inv_mass.reshape(4, ghost), cell_count)
    return filtered, rows.T


def solution(mesh, shape=(NX, NY, NH, NZ)):
    return jax.shard_map(
        functools.partial(local, shape), mesh=mesh,
        in_specs=(P("dom", "band"), P("dom", None, None), P("dom", None), P("dom"), P("dom")),
        out_specs=(P("dom", "band"), P("band", "dom")),
        check_vma=False,
    )
```
